32 devices in a mesh: seq: 4 (over y, x), head: 8 (over z, core).
Axes of the slice: x: 2, y: 2, z: 4, core: 2. Of those that a mesh axis runs over, the one named last changes fastest.
Arguments:
- xraw: bfloat16 [4096, 8192], P('seq', 'head'), may hold values from -6 to 6
- zgate: bfloat16 [4096, 8192], P('seq', 'head'), may hold values from -6 to 6
- bcraw: bfloat16 [4096, 256], P('seq'), may hold values from -6 to 6
- dt: float32 [128, 4096], P('head', 'seq'), may hold values from 6.1035156e-06 to 0.25, as said below
- a_rate: float32 [128], P('head'), may hold values from 1 to 2
- d_skip: float32 [128], P('head'), may hold values from 0.5 to 1.5
- conv_x: float32 [4, 8192], P(None, 'head'), may hold values from -3 to 3
- conv_bc: float32 [4, 256], replicated, may hold values from -3 to 3
- dout: bfloat16 [4096, 8192], P('seq', 'head'), may hold values from -6 to 6
Outputs:
- x_raw_grad: bfloat16 [4096, 8192], P('seq', 'head')
- gate_grad: bfloat16 [4096, 8192], P('seq', 'head')
- step_grad: float32 [128, 4096], P('head', 'seq')
- bc_raw_grad: float32 [4096, 256], P(('seq', 'head'))
- conv_x_grad: float32 [4, 8192], P(None, 'head')
- conv_bc_grad: float32 [4, 256], replicated
The draws below stay inside these ranges and needn't reach their ends.
Inputs may be any that keep to these rules, and one draw needn't show every extreme that they name: `dt`: positive step sizes.
All inputs are finite; a program needn't handle non-finite values.
Results may differ from the reference program's by a relative error of at most 0.028.
Values may be sent and summed in bfloat16 or wider, within the bound.
No kernel may reach another device: no remote copies, remote signals or barrier semaphores. Data moves between devices by JAX's collectives and lax.ppermute only.
A program may use at most 128 MiB of HBM per device.

```python
import math
import jax
import jax.numpy as jnp
from jax import lax

HEADS = 128
HEAD_DIM = 64
STATE = 128
GROUP = 256
CONV = 4
TOKEN_COUNT = 4096


def draw_dt(key, part):
    quick_random_key, random_base_key, jagged_random_key, spike_random_key = jax.random.split(key, 4)
    fast_share = 0.5
    fast_heads = jax.random.uniform(quick_random_key, (HEADS,)) < fast_share
    levels = jax.random.uniform(random_base_key, (HEADS,))
    slow_rate = jnp.exp(jnp.log(0.05) + levels * (jnp.log(0.3) - jnp.log(0.05))) / TOKEN_COUNT
    fast_rate = jnp.exp(jnp.log(1.0 / 60.0) + levels * (jnp.log(1.0 / 25.0) - jnp.log(1.0 / 60.0)))
    base_rate = jnp.where(fast_heads, fast_rate, slow_rate)
    roughness = jax.random.uniform(jagged_random_key, (HEADS, TOKEN_COUNT), minval=0.5, maxval=1.5)
    step_size_values = base_rate[:, None] * roughness
    spike_positions_list = jax.random.randint(spike_random_key, (3,), 0, TOKEN_COUNT)
    spike_mask = jnp.any(jnp.arange(TOKEN_COUNT, dtype=jnp.int32)[None, :] == spike_positions_list[:, None], axis=0)
    return jnp.where(spike_mask[None, :], 0.25, step_size_values).astype(jnp.float32)


def steps_of(own_key, dims, cuts, low, high):
    def one(axis_at, blocks):
        steps = jax.random.uniform(jax.random.fold_in(jax.random.fold_in(own_key, 6), axis_at), (blocks,), jnp.float32, low / len(cuts), high / len(cuts))
        return jnp.repeat(jnp.exp(steps), dims[axis_at] // blocks).reshape((-1,) + (1,) * (len(dims) - axis_at - 1))

    level = one(*cuts[0])
    for cut in cuts[1:]:
        level = level * one(*cut)
    return level


def scatter_about(stream_key, shape, width, limit, shards=(), kind=jnp.bfloat16):
    entries = width * jax.random.normal(stream_key, shape, jnp.float32)
    if shards:
        entries = entries * steps_of(stream_key, shape, shards, -0.22, 0.18)
    return jnp.clip(entries, -limit, limit).astype(kind)


def setup_inputs(seed: int = 0) -> dict:
    streams_of = jax.random.split(jax.random.key(seed), 10)
    xraw = scatter_about(streams_of[0], (TOKEN_COUNT, HEADS * HEAD_DIM), 1.0, 6.0, ((0, 4), (1, 8)))
    zgate = scatter_about(streams_of[1], (TOKEN_COUNT, HEADS * HEAD_DIM), 1.0, 6.0, ((0, 4), (1, 8)))
    bcraw = scatter_about(streams_of[2], (TOKEN_COUNT, 2 * STATE), 1.0, 6.0, ((0, 4),))
    dt = draw_dt(jax.random.fold_in(streams_of[9], 71), 0)
    a_rate = jnp.clip(jnp.exp(math.log(2.0) - 0.6931472 * jax.random.uniform(streams_of[4], (HEADS,), jnp.float32) ** steps_of(streams_of[4], (HEADS,), ((0, 8),), -0.2, 0.2)), 1.0, 2.0)
    d_skip = jnp.clip(0.5 + 1.0 * jax.random.uniform(streams_of[5], (HEADS,), jnp.float32) ** steps_of(streams_of[5], (HEADS,), ((0, 8),), -0.2, 0.2), 0.5, 1.5)
    conv_x = scatter_about(streams_of[6], (CONV, HEADS * HEAD_DIM), CONV ** -0.5, 3.0, ((1, 8),), jnp.float32)
    conv_bc = scatter_about(streams_of[7], (CONV, 2 * STATE), CONV ** -0.5, 3.0, (), jnp.float32)
    dout = scatter_about(streams_of[8], (TOKEN_COUNT, HEADS * HEAD_DIM), 1.0, 6.0, ((0, 4), (1, 8)))
    return {"xraw": xraw, "zgate": zgate, "bcraw": bcraw, "dt": dt, "a_rate": a_rate, "d_skip": d_skip, "conv_x": conv_x, "conv_bc": conv_bc, "dout": dout}


def silu_slope(values):
    logistic = jax.nn.sigmoid(values)
    return logistic * (1.0 + values * (1.0 - logistic))

def conv_apply(extended, weight, length):
    conv_len = weight.shape[0]
    running = jnp.zeros((length, extended.shape[1]), jnp.float32)
    for offset in range(conv_len):
        start_row = conv_len - 1 - offset
        running = running + weight[offset][None, :] * extended[start_row:start_row + length].astype(jnp.float32)
    return running

def conv_adjoint(extended, weight, length):
    conv_len = weight.shape[0]
    running = jnp.zeros((length, extended.shape[1]), jnp.float32)
    for offset in range(conv_len):
        running = running + weight[offset][None, :] * extended[offset:offset + length]
    return running

def conv_weight_grad(slope_rows, raw_extended, conv_len):
    length = slope_rows.shape[0]
    rows_list = []
    for offset in range(conv_len):
        start_row = conv_len - 1 - offset
        rows_list.append(lax.optimization_barrier(jnp.sum(slope_rows * raw_extended[start_row:start_row + length].astype(jnp.float32), axis=0)))
    return jnp.stack(rows_list)

def pair_decay(within_block):
    block_len = within_block.shape[-1]
    places = jnp.arange(block_len, dtype=jnp.int32)
    causal = (places[:, None] >= places[None, :]).astype(jnp.float32)
    return jnp.exp(jnp.minimum(within_block[..., None, :] - within_block[..., :, None], 0.0)) * causal

def block_tables(b_b, c_b, within_b):
    totals_b = within_b[:, -1]
    decay_b = pair_decay(within_b)
    scores = jnp.dot(c_b, b_b.T, preferred_element_type=jnp.float32)
    kernel = (scores[None] * decay_b).astype(jnp.bfloat16)
    enter = jnp.exp(-within_b).T[:, :, None]
    leave = jnp.exp(-(totals_b[:, None] - within_b)).T[:, :, None]
    return (totals_b, decay_b, kernel, enter, leave)

def reference(xraw, zgate, bcraw, dt, a_rate, d_skip, conv_x, conv_bc, dout):
    length = xraw.shape[0]
    head_count = HEADS
    head_size = HEAD_DIM
    state_dim = STATE
    block_len = GROUP
    block_count = length // block_len
    conv_len = CONV
    x_extended = jnp.pad(xraw, ((conv_len - 1, 0), (0, 0)))
    bc_extended = jnp.pad(bcraw, ((conv_len - 1, 0), (0, 0)))
    x_post = jax.nn.silu(conv_apply(x_extended, conv_x, length)).astype(jnp.bfloat16)
    bc_pre = conv_apply(bc_extended, conv_bc, length)
    bc_post = jax.nn.silu(bc_pre).astype(jnp.bfloat16)
    b_blocks = bc_post[:, :state_dim].reshape(block_count, block_len, state_dim)
    c_blocks = bc_post[:, state_dim:].reshape(block_count, block_len, state_dim)
    x_blocks = x_post.reshape(block_count, block_len, head_count, head_size)
    step_blocks = dt.reshape(head_count, block_count, block_len).transpose(1, 0, 2)
    within = jnp.cumsum(a_rate[None, :, None] * step_blocks, axis=2)
    w_blocks = (x_blocks.astype(jnp.float32) * step_blocks.transpose(0, 2, 1)[..., None]).astype(jnp.bfloat16)
    gate_blocks = zgate.reshape(block_count, block_len, head_count, head_size)
    dout_blocks = dout.reshape(block_count, block_len, head_count, head_size)

    def forward_block(carried, pieces):
        x_b, w_b, b_b, c_b, within_b, gate_b, dout_b = pieces
        totals_b, decay_b, kernel, enter, leave = block_tables(b_b, c_b, within_b)
        states_bf = carried.astype(jnp.bfloat16)
        inner_part = jnp.einsum('hts,shp->thp', kernel.astype(jnp.float32), w_b.astype(jnp.float32))
        outer_part = jnp.einsum('tn,hpn->thp', c_b.astype(jnp.float32), states_bf.astype(jnp.float32)) * enter
        output_y = inner_part + outer_part + d_skip[None, :, None] * x_b.astype(jnp.float32)
        gate_f = gate_b.astype(jnp.float32)
        gate_grad = (dout_b.astype(jnp.float32) * output_y * silu_slope(gate_f)).astype(jnp.bfloat16)
        w_leave = (w_b.astype(jnp.float32) * leave).astype(jnp.bfloat16)
        ends = jnp.einsum('shp,sn->hpn', w_leave.astype(jnp.float32), b_b.astype(jnp.float32))
        carried = jnp.exp(-totals_b)[:, None, None] * carried + ends
        return (carried, (states_bf, gate_grad))
    start_state = jnp.zeros((head_count, head_size, state_dim), jnp.float32)
    unused, (states_all, gate_all) = lax.scan(forward_block, start_state, (x_blocks, w_blocks, b_blocks, c_blocks, within, gate_blocks, dout_blocks))

    def backward_block(carried, pieces):
        x_b, w_b, b_b, c_b, within_b, gate_b, dout_b, step_b, states_bf = pieces
        totals_b, decay_b, kernel, enter, leave = block_tables(b_b, c_b, within_b)
        grads_bf = carried.astype(jnp.bfloat16)
        dy_bf = (dout_b.astype(jnp.float32) * jax.nn.silu(gate_b.astype(jnp.float32))).astype(jnp.bfloat16)
        dy_f = dy_bf.astype(jnp.float32)
        dy_enter = (dy_f * enter).astype(jnp.bfloat16)
        w_f = w_b.astype(jnp.float32)
        w_grad = jnp.einsum('hts,thp->shp', kernel.astype(jnp.float32), dy_f) + leave * jnp.einsum('sn,hpn->shp', b_b.astype(jnp.float32), grads_bf.astype(jnp.float32))
        x_grad = step_b.T[:, :, None] * w_grad + d_skip[None, :, None] * dy_f
        step_grad = lax.optimization_barrier(jnp.sum(x_b.astype(jnp.float32) * w_grad, axis=2))
        mixing = jnp.einsum('thp,shp->hts', dy_f, w_f)
        mixed = lax.optimization_barrier(jnp.sum(mixing * decay_b, axis=0)).astype(jnp.bfloat16)
        c_grad = jnp.dot(mixed, b_b, preferred_element_type=jnp.float32) + lax.optimization_barrier(jnp.sum(enter * jnp.einsum('thp,hpn->thn', dy_f, states_bf.astype(jnp.float32)), axis=1))
        b_grad = jnp.dot(mixed.T, c_b, preferred_element_type=jnp.float32) + lax.optimization_barrier(jnp.sum(leave * jnp.einsum('shp,hpn->shn', w_f, grads_bf.astype(jnp.float32)), axis=1))
        starts_grad = jnp.einsum('thp,tn->hpn', dy_enter.astype(jnp.float32), c_b.astype(jnp.float32))
        carried = jnp.exp(-totals_b)[:, None, None] * carried + starts_grad
        return (carried, (x_grad, step_grad, jnp.concatenate([b_grad, c_grad], axis=-1)))
    unused_grad, (x_grads, step_grads, shared) = lax.scan(backward_block, start_state, (x_blocks, w_blocks, b_blocks, c_blocks, within, gate_blocks, dout_blocks, step_blocks, states_all), reverse=True)
    x_pre = conv_apply(x_extended, conv_x, length)
    x_slope = x_grads.reshape(length, head_count * head_size) * silu_slope(x_pre)
    x_raw_grad = conv_adjoint(jnp.pad(x_slope, ((0, conv_len - 1), (0, 0))), conv_x, length).astype(jnp.bfloat16)
    conv_x_grad = conv_weight_grad(x_slope, x_extended, conv_len)
    bc_slope = shared.reshape(length, 2 * state_dim) * silu_slope(bc_pre)
    bc_raw_grad = conv_adjoint(jnp.pad(bc_slope, ((0, conv_len - 1), (0, 0))), conv_bc, length)
    conv_bc_grad = conv_weight_grad(bc_slope, bc_extended, conv_len)
    step_grad = step_grads.reshape(length, head_count).T
    gate_grad = gate_all.reshape(length, head_count * head_size)
    return (x_raw_grad, gate_grad, step_grad, bc_raw_grad, conv_x_grad, conv_bc_grad)
```

```python
import functools

import jax
import jax.numpy as jnp
from jax import lax
from jax.experimental import pallas as pl
from jax.experimental.pallas import tpu as pltpu
from jax.sharding import PartitionSpec as P

HEAD_DIM = 64
GROUP = 256
HEADS_AT_ONCE = 4
WIDE = HEAD_DIM * HEADS_AT_ONCE
SUB = 64
EDGE = 8
F32 = jnp.float32
BF16 = jnp.bfloat16


def shifted(value, axis, steps):
    count = lax.axis_size(axis)
    return lax.ppermute(value, axis, [(i, (i + steps) % count) for i in range(count)])


def from_behind(value, axis, steps):
    count = lax.axis_size(axis)
    first, last = (max(0, -steps), min(count, count - steps))
    return lax.ppermute(value, axis, [(i, i + steps) for i in range(first, last)])


def sum_over(value, axis):
    count = lax.axis_size(axis)
    parts = [value] + [
        lax.ppermute(value, axis, [(i, i ^ k) for i in range(count)]) for k in range(1, count)
    ]
    while len(parts) > 1:
        parts = [a + b for a, b in zip(parts[::2], parts[1::2])]
    return parts[0]


def dot(a, b):
    return jnp.dot(a, b, preferred_element_type=F32)


def dot_t(a, b):
    return lax.dot_general(a, b, (((1,), (1,)), ((), ())), preferred_element_type=F32)


def dot_tn(a, b):
    return lax.dot_general(a, b, (((0,), (0,)), ((), ())), preferred_element_type=F32)


def logistic(v):
    return 0.5 + 0.5 * jnp.tanh(0.5 * v)


def running_sum(g):
    place = lax.broadcasted_iota(jnp.int32, g.shape, 1) % GROUP
    step = 1
    while step < GROUP:
        g = g + jnp.where(place >= step, pltpu.roll(g, step, axis=1), 0.0)
        step *= 2
    return g


def token_scales(within, steps, k):
    w = within[:, k * GROUP : (k + 1) * GROUP]
    d = steps[:, k * GROUP : (k + 1) * GROUP]
    total = w[:, GROUP - 1 : GROUP]
    upper = lax.broadcasted_iota(jnp.int32, w.shape, 0) < HEADS_AT_ONCE
    gap = w - 0.5 * total
    e = jnp.exp(jnp.where(upper, gap, -gap))
    return e, jnp.where(upper, e * d, e).T, total


def over_lanes(columns, first):
    rows = columns.shape[0]
    left = lax.broadcasted_iota(jnp.int32, (rows, 2 * HEAD_DIM), 1) < HEAD_DIM
    c = [
        jnp.broadcast_to(columns[:, first + j : first + j + 1], (rows, 2 * HEAD_DIM))
        for j in range(HEADS_AT_ONCE)
    ]
    return jnp.concatenate(
        [jnp.where(left, c[j], c[j + 1]) for j in range(0, HEADS_AT_ONCE, 2)], axis=1
    )


def head_row(total):
    lane = lax.broadcasted_iota(jnp.int32, (1, WIDE), 1)
    row = jnp.broadcast_to(total[0:1], (1, WIDE))
    for j in range(1, HEADS_AT_ONCE):
        row = jnp.where(lane >= j * HEAD_DIM, jnp.broadcast_to(total[j : j + 1], (1, WIDE)), row)
    return row


def load_extended(ext, rim, body):
    ext[0:EDGE, :] = rim[...].astype(F32)
    ext[EDGE:, :] = body[...].astype(F32)


def conv_rows(ext, taps, start, rows):
    out = taps[0:1, :] * ext[EDGE + start : EDGE + start + rows, :]
    for k in range(1, taps.shape[0]):
        out = out + taps[k : k + 1, :] * ext[EDGE + start - k : EDGE + start - k + rows, :]
    return out


def silu_slope(v):
    q = logistic(v)
    return q * (1.0 + v * (1.0 - q))


def first_kernel(
    count, place, rim_x, rim_bc, x, z, up, bcraw, dt, rate, taps, bc_taps,
    w_out, d_out, bc_out, lower, upper, states, grads, *rest,
):
    sends = rest[: count - 1]
    ext, bc_ext, bct, ctd = rest[count - 1 :]
    length = x.shape[0]
    blocks = length // GROUP
    n = bcraw.shape[1] // 2

    @pl.when(pl.program_id(0) == 0)
    def _():
        load_extended(bc_ext, rim_bc, bcraw)
        r = lax.broadcasted_iota(jnp.int32, (GROUP, GROUP), 0)
        c = lax.broadcasted_iota(jnp.int32, (GROUP, GROUP), 1)
        for k in range(blocks):
            rows = slice(k * GROUP, (k + 1) * GROUP)
            pre = conv_rows(bc_ext, bc_taps, k * GROUP, GROUP)
            post = (pre * logistic(pre)).astype(BF16)
            bc_out[rows, :] = post
            post_t = post.astype(F32).T.astype(BF16)
            bct[k] = post_t
            lower[k] = jnp.where(r >= c, dot(post[:, n:], post_t[:n]), 0.0).astype(BF16)
            upper[k] = jnp.where(r <= c, dot(post[:, :n], post_t[n:]), 0.0).astype(BF16)

    load_extended(ext, rim_x, x)
    steps = dt[0]
    within = running_sum(rate[0] * steps)
    state = jnp.zeros((n, WIDE), F32)
    totals = []
    for k in range(blocks):
        _, columns, total = token_scales(within, steps, k)
        for s in range(0, GROUP, SUB):
            here = k * GROUP + s
            rows = slice(here, here + SUB)
            pre = conv_rows(ext, taps, here, SUB)
            post = (pre * logistic(pre)).astype(BF16).astype(F32)
            w_out[rows, :] = (over_lanes(columns[s : s + SUB], 0) * post).astype(BF16)
            gate = z[rows, :].astype(F32)
            dy = (up[rows, :].astype(F32) * (gate * logistic(gate))).astype(BF16).astype(F32)
            d_out[rows, :] = (over_lanes(columns[s : s + SUB], HEADS_AT_ONCE) * dy).astype(BF16)
        rows = slice(k * GROUP, (k + 1) * GROUP)
        total = head_row(total)
        totals.append(total)
        states[k] = state.astype(BF16)
        half = jnp.exp(-0.5 * total)
        state = jnp.exp(-total) * state + half * dot(bct[k, :n, :], w_out[rows, :])
        ctd[k] = half * dot(bct[k, n:, :], d_out[rows, :])
    grad = jnp.zeros((n, WIDE), F32)
    for k in reversed(range(blocks)):
        grads[k] = grad.astype(BF16)
        grad = jnp.exp(-totals[k]) * grad + ctd[k]
    whole = sum(totals[1:], totals[0])
    high = whole.astype(BF16).astype(F32)
    mid = (whole - high).astype(BF16).astype(F32)
    low = whole - high - mid
    r = lax.broadcasted_iota(jnp.int32, (16, WIDE), 0)
    extra = jnp.where(r == 0, high, jnp.where(r == 1, mid, jnp.where(r == 2, low, 0.0))).astype(BF16)
    for k in range(1, count):
        onward = place[0] + k < count
        sends[k - 1][0:n, :] = jnp.where(onward, state, grad).astype(BF16)
        sends[k - 1][n:, :] = extra


def inner_kernel(
    rim_x, x, z, up, dt, rate, taps, skip, w, d, bc, lower, upper,
    gate_base, gate_scale, slope_base, slope_scale, post_out, step_out, bc_part, ext, mix,
):
    length = x.shape[0]
    blocks = length // GROUP
    n = bc.shape[1] // 2
    chunk = pl.program_id(0)
    load_extended(ext, rim_x, x)
    steps = dt[0]
    within = running_sum(rate[0] * steps)
    picks = (
        lax.broadcasted_iota(jnp.int32, (2 * HEADS_AT_ONCE, WIDE), 1) // HEAD_DIM
        == lax.broadcasted_iota(jnp.int32, (2 * HEADS_AT_ONCE, WIDE), 0)
    ).astype(BF16)
    for k in range(blocks):
        rows = slice(k * GROUP, (k + 1) * GROUP)
        e, columns, _ = token_scales(within, steps, k)
        y0 = dot(lower[k], w[rows, :])
        p0 = dot(upper[k], d[rows, :])
        fresh = dot_t(d[rows, :], w[rows, :])

        @pl.when(chunk == 0)
        def _():
            mix[k] = fresh

        @pl.when(chunk > 0)
        def _():
            mix[k] += fresh

        highs, lows = [], []
        for s in range(0, GROUP, SUB):
            here = k * GROUP + s
            sub = slice(here, here + SUB)
            part = slice(s, s + SUB)
            pre = conv_rows(ext, taps, here, SUB)
            q = logistic(pre)
            slope = q * (1.0 + pre * (1.0 - q))
            post_b = (pre * q).astype(BF16)
            post = post_b.astype(F32)
            post_out[sub, :] = post_b
            gate = z[sub, :].astype(F32)
            qz = logistic(gate)
            upstream = up[sub, :].astype(F32)
            dy = (upstream * (gate * qz)).astype(BF16).astype(F32)
            gz = upstream * (qz * (1.0 + gate * (1.0 - qz)))
            ud = over_lanes(columns[part], 0)
            v = over_lanes(columns[part], HEADS_AT_ONCE)
            gv = gz * v
            gate_base[sub, :] = (gv * y0[part] + gz * (skip[...] * post)).astype(BF16)
            gate_scale[sub, :] = gv.astype(BF16)
            su = slope * ud
            slope_base[sub, :] = (su * p0[part] + slope * (skip[...] * dy)).astype(BF16)
            slope_scale[sub, :] = su.astype(BF16)
            q0 = post * p0[part]
            high = q0.astype(BF16)
            highs.append(high)
            lows.append((q0 - high.astype(F32)).astype(BF16))
        st = dot_t(picks, jnp.concatenate(highs, 0)) + dot_t(picks, jnp.concatenate(lows, 0))
        step_out[0, :, rows] = st

    @pl.when(chunk == pl.num_programs(0) - 1)
    def _():
        r = lax.broadcasted_iota(jnp.int32, (GROUP, GROUP), 0)
        c = lax.broadcasted_iota(jnp.int32, (GROUP, GROUP), 1)
        for k in range(blocks):
            rows = slice(k * GROUP, (k + 1) * GROUP)
            m = jnp.where(r >= c, mix[k], 0.0)
            bc_part[rows, n:] = dot(m.astype(BF16), bc[rows, :n])
            bc_part[rows, :n] = dot(m.T.astype(BF16), bc[rows, n:])


def shared_kernel(
    count, shares, place, rim_bc, bcraw, bc_taps, dt, rate, w, d, states, grads, bc_part, *rest,
):
    gets = rest[: count - 1]
    s_out, g_out, own, own_slope, tap_part = rest[count - 1 : count + 4]
    sends = rest[count + 4 : count + 3 + shares]
    acc, bc_ext, slopes = rest[count + 3 + shares :]
    length = w.shape[0]
    blocks = length // GROUP
    n = bcraw.shape[1] // 2
    chunk = pl.program_id(0)

    @pl.when(chunk == 0)
    def _():
        acc[...] = bc_part[...]

    within = running_sum(rate[0] * dt[0])
    state_in = jnp.zeros((n, WIDE), F32)
    grad_in = jnp.zeros((n, WIDE), F32)
    spans = [None] + [
        sum(get[n + j : n + j + 1, :].astype(F32) for j in range(3)) for get in gets
    ]
    gone = jnp.zeros((1, WIDE), F32)
    for k in range(1, count):
        weight = jnp.where(place[0] >= k, jnp.exp(-gone), 0.0)
        state_in = state_in + weight * gets[k - 1][0:n, :].astype(F32)
        gone = gone + spans[k]
    gone = jnp.zeros((1, WIDE), F32)
    for ahead in range(1, count):
        k = count - ahead
        weight = jnp.where(place[0] < k, jnp.exp(-gone), 0.0)
        grad_in = grad_in + weight * gets[k - 1][0:n, :].astype(F32)
        gone = gone + spans[k]
    totals = [
        head_row(within[:, (k + 1) * GROUP - 1 : (k + 1) * GROUP]) for k in range(blocks)
    ]
    gone = jnp.zeros((1, WIDE), F32)
    for k in range(blocks):
        rows = slice(k * GROUP, (k + 1) * GROUP)
        half = jnp.exp(-0.5 * totals[k])
        later = sum(totals[k + 1 :], jnp.zeros((1, WIDE), F32))
        sk = (half * (states[k].astype(F32) + jnp.exp(-gone) * state_in)).astype(BF16)
        gk = (half * (grads[k].astype(F32) + jnp.exp(-later) * grad_in)).astype(BF16)
        gone = gone + totals[k]
        s_out[k] = sk
        g_out[k] = gk
        acc[rows, n:] += dot_t(d[rows, :], sk)
        acc[rows, :n] += dot_t(w[rows, :], gk)

    @pl.when(chunk == pl.num_programs(0) - 1)
    def _():
        load_extended(bc_ext, rim_bc, bcraw)
        taps = bc_taps.shape[0]
        sums = [jnp.zeros((1, 2 * n), F32) for _ in range(taps)]
        for s in range(0, length, SUB):
            slope = silu_slope(conv_rows(bc_ext, bc_taps, s, SUB))
            slopes[s : s + SUB, :] = slope
            full = slope * acc[s : s + SUB, :]
            for k in range(taps):
                sums[k] = sums[k] + jnp.sum(
                    full * bc_ext[EDGE + s - k : EDGE + s - k + SUB, :], axis=0, keepdims=True
                )
        for k in range(taps):
            tap_part[k : k + 1, :] = sums[k]
        share = length // shares
        mine = place[1]
        start = pl.multiple_of(mine * share, share)
        own[...] = acc[pl.ds(start, share), :]
        own_slope[...] = slopes[pl.ds(start, share), :]
        for k in range(1, shares):
            start = pl.multiple_of(lax.rem(mine + k, shares) * share, share)
            sends[k - 1][...] = acc[pl.ds(start, share), :].astype(BF16)


def outer_kernel(
    rim_x, x, dt, rate, taps, gate_base, gate_scale, slope_base, slope_scale, post,
    step_part, bc, s_in, g_in,
    gate_out, x_out, step_out, tap_part, head_rows, tail_rows, ext, slope_ext,
):
    length = x.shape[0]
    blocks = length // GROUP
    n = bc.shape[1] // 2
    load_extended(ext, rim_x, x)
    steps = dt[0]
    within = running_sum(rate[0] * steps)
    picks = (
        lax.broadcasted_iota(jnp.int32, (2 * HEADS_AT_ONCE, WIDE), 1) // HEAD_DIM
        == lax.broadcasted_iota(jnp.int32, (2 * HEADS_AT_ONCE, WIDE), 0)
    ).astype(BF16)
    count = taps.shape[0]
    sums = [jnp.zeros((1, WIDE), F32) for _ in range(count)]
    slope_ext[length : length + EDGE, :] = jnp.zeros((EDGE, WIDE), F32)
    for k in range(blocks):
        rows = slice(k * GROUP, (k + 1) * GROUP)
        e, _, _ = token_scales(within, steps, k)
        y1 = dot(bc[rows, n:], s_in[k])
        p1 = dot(bc[rows, :n], g_in[k])
        highs, lows = [], []
        for s in range(0, GROUP, SUB):
            here = k * GROUP + s
            sub = slice(here, here + SUB)
            part = slice(s, s + SUB)
            gate_out[sub, :] = (
                gate_base[sub, :].astype(F32) + gate_scale[sub, :].astype(F32) * y1[part]
            ).astype(BF16)
            slope = slope_base[sub, :].astype(F32) + slope_scale[sub, :].astype(F32) * p1[part]
            slope_ext[sub, :] = slope
            for j in range(count):
                sums[j] = sums[j] + jnp.sum(
                    slope * ext[EDGE + here - j : EDGE + here - j + SUB, :], axis=0, keepdims=True
                )
            q1 = post[sub, :].astype(F32) * p1[part]
            high = q1.astype(BF16)
            highs.append(high)
            lows.append((q1 - high.astype(F32)).astype(BF16))
        st = dot_t(picks, jnp.concatenate(highs, 0)) + dot_t(picks, jnp.concatenate(lows, 0))
        step_out[0, :, rows] = e * (st + step_part[0, :, rows])
    for j in range(count):
        tap_part[j : j + 1, :] = sums[j]
    head_rows[...] = slope_ext[0:EDGE, :]
    for s in range(0, length, SUB):
        out = taps[0:1, :] * slope_ext[s : s + SUB, :]
        for j in range(1, count):
            out = out + taps[j : j + 1, :] * slope_ext[s + j : s + j + SUB, :]
        x_out[s : s + SUB, :] = out.astype(BF16)
        if s + SUB == length:
            tail_rows[...] = out[SUB - 2 * EDGE :]


def local(xraw, zgate, bcraw, dt, a_rate, d_skip, conv_x, conv_bc, dout):
    length, channels = xraw.shape
    heads = a_rate.shape[0]
    n2 = bcraw.shape[1]
    n = n2 // 2
    taps = conv_x.shape[0]
    blocks = length // GROUP
    chunks = channels // WIDE
    count = lax.axis_size("seq")
    shares = lax.axis_size("head")
    share = length // shares
    place = jnp.stack([lax.axis_index("seq"), lax.axis_index("head")]).astype(jnp.int32)
    dt_pairs = dt.reshape(chunks, HEADS_AT_ONCE, length)
    dt_pairs = jnp.concatenate([dt_pairs, dt_pairs], axis=1)
    rates = a_rate.reshape(chunks, HEADS_AT_ONCE, 1)
    rates = jnp.concatenate([rates, rates], axis=1)
    skips = jnp.repeat(d_skip, channels // heads)[None, :]
    before = from_behind(
        jnp.concatenate([xraw[length - EDGE :], bcraw[length - EDGE :]], axis=1), "seq", 1
    )
    before_x, before_bc = before[:, :channels], before[:, channels:]

    tall = pl.BlockSpec((length, WIDE), lambda c: (0, c))
    edge = pl.BlockSpec((EDGE, WIDE), lambda c: (0, c))
    tap = pl.BlockSpec((taps, WIDE), lambda c: (0, c))
    row = pl.BlockSpec((1, WIDE), lambda c: (0, c))
    pair = pl.BlockSpec((1, 2 * HEADS_AT_ONCE, length), lambda c: (c, 0, 0))
    rate = pl.BlockSpec((1, 2 * HEADS_AT_ONCE, 1), lambda c: (c, 0, 0))
    state = pl.BlockSpec((blocks, n, WIDE), lambda c: (0, 0, c))
    carry = pl.BlockSpec((n + 16, WIDE), lambda c: (0, c))
    scalar = pl.BlockSpec(memory_space=pltpu.SMEM)

    def fixed(*shape):
        return pl.BlockSpec(shape, lambda c: (0,) * len(shape))

    def arr(shape, dtype):
        return jax.ShapeDtypeStruct(shape, dtype)

    params = pltpu.CompilerParams(
        dimension_semantics=("arbitrary",), vmem_limit_bytes=48 * 1024 * 1024
    )
    wide = arr((length, channels), BF16)
    square = (blocks, GROUP, GROUP)
    stack = arr((blocks, n, channels), BF16)
    first = pl.pallas_call(
        functools.partial(first_kernel, count),
        grid=(chunks,),
        in_specs=[scalar, edge, fixed(EDGE, n2), tall, tall, tall, fixed(length, n2), pair, rate,
                  tap, fixed(taps, n2)],
        out_specs=[tall, tall, fixed(length, n2), fixed(*square), fixed(*square), state, state]
        + [carry] * (count - 1),
        out_shape=[wide, wide, arr((length, n2), BF16), arr(square, BF16), arr(square, BF16),
                   stack, stack] + [arr((n + 16, channels), BF16)] * (count - 1),
        scratch_shapes=[
            pltpu.VMEM((length + EDGE, WIDE), F32),
            pltpu.VMEM((length + EDGE, n2), F32),
            pltpu.VMEM((blocks, n2, GROUP), BF16),
            pltpu.VMEM((blocks, n, WIDE), F32),
        ],
        compiler_params=params,
        name="first",
    )(place, before_x, before_bc, xraw, zgate, dout, bcraw, dt_pairs, rates, conv_x, conv_bc)
    w, d, bc, lower, upper, states, grads = first[:7]
    gets = [shifted(sent, "seq", k + 1) for k, sent in enumerate(first[7:])]

    inner = pl.pallas_call(
        inner_kernel,
        grid=(chunks,),
        in_specs=[edge, tall, tall, tall, pair, rate, tap, row, tall, tall, fixed(length, n2),
                  fixed(*square), fixed(*square)],
        out_specs=[tall] * 5 + [pair, fixed(length, n2)],
        out_shape=[wide] * 5 + [arr(dt_pairs.shape, F32), arr((length, n2), F32)],
        scratch_shapes=[pltpu.VMEM((length + EDGE, WIDE), F32), pltpu.VMEM(square, F32)],
        compiler_params=params,
        cost_estimate=pl.CostEstimate(
            flops=40_000_000_000, transcendentals=0, bytes_accessed=30_000_000
        ),
        name="inner",
    )(before_x, xraw, zgate, dout, dt_pairs, rates, conv_x, skips, w, d, bc, lower, upper)
    gate_base, gate_scale, slope_base, slope_scale, post, step_part, bc_part = inner

    shared = pl.pallas_call(
        functools.partial(shared_kernel, count, shares),
        grid=(chunks,),
        in_specs=[scalar, fixed(EDGE, n2), fixed(length, n2), fixed(taps, n2), pair, rate, tall,
                  tall, state, state, fixed(length, n2)] + [carry] * (count - 1),
        out_specs=[state, state, fixed(share, n2), fixed(share, n2), fixed(taps, n2)]
        + [fixed(share, n2)] * (shares - 1),
        out_shape=[stack, stack, arr((share, n2), F32), arr((share, n2), F32),
                   arr((taps, n2), F32)] + [arr((share, n2), BF16)] * (shares - 1),
        scratch_shapes=[
            pltpu.VMEM((length, n2), F32),
            pltpu.VMEM((length + EDGE, n2), F32),
            pltpu.VMEM((length, n2), F32),
        ],
        compiler_params=params,
        name="shared",
    )(place, before_bc, bcraw, conv_bc, dt_pairs, rates, w, d, states, grads, bc_part, *gets)
    s_in, g_in, own, own_slope, bc_taps_part = shared[:5]
    own_parts = [shifted(sent, "head", k + 1) for k, sent in enumerate(shared[5:])]

    outer = pl.pallas_call(
        outer_kernel,
        grid=(chunks,),
        in_specs=[edge, tall, pair, rate, tap, tall, tall, tall, tall, tall, pair,
                  fixed(length, n2), state, state],
        out_specs=[tall, tall, pair, tap, edge, pl.BlockSpec((2 * EDGE, WIDE), lambda c: (0, c))],
        out_shape=[wide, wide, arr(dt_pairs.shape, F32), arr((taps, channels), F32),
                   arr((EDGE, channels), F32), arr((2 * EDGE, channels), F32)],
        scratch_shapes=[pltpu.VMEM((length + EDGE, WIDE), F32)] * 2,
        compiler_params=params,
        cost_estimate=pl.CostEstimate(
            flops=40_000_000_000, transcendentals=0, bytes_accessed=30_000_000
        ),
        name="outer",
    )(before_x, xraw, dt_pairs, rates, conv_x, gate_base, gate_scale, slope_base, slope_scale,
      post, step_part, bc, s_in, g_in)
    gate_grad, x_raw_grad, step_pairs, x_taps_part, head_rows, tail_rows = outer

    step_grad = step_pairs[:, :HEADS_AT_ONCE].reshape(heads, length)
    bc_over_heads = sum_over(bc_taps_part, "head")
    own_rows = sum((part.astype(F32) for part in own_parts), own) * own_slope
    next_rows = from_behind(own_rows[:EDGE], ("seq", "head"), -1)
    own_ext = jnp.concatenate([own_rows, next_rows], axis=0)
    bc_raw_grad = sum(conv_bc[k][None] * own_ext[k : k + share] for k in range(taps))
    x_next = from_behind(head_rows, "seq", -1)
    pad = jnp.concatenate([jnp.zeros((2 * EDGE, channels), F32), x_next], axis=0)
    tail = tail_rows + sum(conv_x[k][None] * pad[k : k + 2 * EDGE] for k in range(1, taps))
    x_raw_grad = lax.dynamic_update_slice(
        x_raw_grad, tail.astype(BF16), (length - 2 * EDGE, 0)
    )
    tap_sums = sum_over(jnp.concatenate([x_taps_part, bc_over_heads], axis=1), "seq")
    return (x_raw_grad, gate_grad, step_grad, bc_raw_grad, tap_sums[:, :channels],
            tap_sums[:, channels:])


def solution(mesh):
    placed = (
        P("seq", "head"),
        P("seq", "head"),
        P("seq", None),
        P("head", "seq"),
        P("head"),
        P("head"),
        P(None, "head"),
        P(),
        P("seq", "head"),
    )
    return jax.shard_map(
        local,
        mesh=mesh,
        in_specs=placed,
        out_specs=(
            P("seq", "head"),
            P("seq", "head"),
            P("head", "seq"),
            P(("seq", "head"), None),
            P(None, "head"),
            P(),
        ),
        check_vma=False,
    )
```

```python
import functools

import jax
import jax.numpy as jnp
from jax import lax
from jax.experimental import pallas as pl
from jax.experimental.pallas import tpu as pltpu
from jax.sharding import PartitionSpec as P

HEAD_DIM = 64
GROUP = 256
HEADS_AT_ONCE = 4
WIDE = HEAD_DIM * HEADS_AT_ONCE
LANES = 2 * HEAD_DIM
HALVES = HEADS_AT_ONCE // 2
SUB = 128
EDGE = 8
RIM = 16
F32 = jnp.float32
BF16 = jnp.bfloat16


def shifted(value, axis, steps):
    count = lax.axis_size(axis)
    return lax.ppermute(value, axis, [(i, (i + steps) % count) for i in range(count)])


def from_behind(value, axis, steps):
    count = lax.axis_size(axis)
    first, last = (max(0, -steps), min(count, count - steps))
    return lax.ppermute(value, axis, [(i, i + steps) for i in range(first, last)])


def swapped(value, axis, k):
    return lax.ppermute(value, axis, [(i, i ^ k) for i in range(lax.axis_size(axis))])


def tree_sum(parts):
    while len(parts) > 1:
        parts = [a + b for a, b in zip(parts[::2], parts[1::2])]
    return parts[0]


def sum_over(value, axis):
    k = 1
    while k < lax.axis_size(axis):
        value = value + swapped(value, axis, k)
        k *= 2
    return value


def dot(a, b):
    return jnp.dot(a, b, preferred_element_type=F32)


def dot_t(a, b):
    return lax.dot_general(a, b, (((1,), (1,)), ((), ())), preferred_element_type=F32)


def running_sum(g):
    place = lax.broadcasted_iota(jnp.int32, g.shape, 1) % GROUP
    step = 1
    while step < GROUP:
        g = g + jnp.where(place >= step, pltpu.roll(g, step, axis=1), 0.0)
        step *= 2
    return g


def token_gaps(within, k):
    w = within[:, k * GROUP : (k + 1) * GROUP]
    total = w[:, GROUP - 1 : GROUP]
    return w - 0.5 * total, total


def token_columns(within, steps, k):
    gap, total = token_gaps(within, k)
    upper = lax.broadcasted_iota(jnp.int32, gap.shape, 0) < HEADS_AT_ONCE
    e = jnp.exp(jnp.where(upper, gap, -gap))
    return jnp.where(upper, e * steps[:, k * GROUP : (k + 1) * GROUP], e).T, total


def over_lanes(columns, first, h):
    rows = columns.shape[0]
    left = lax.broadcasted_iota(jnp.int32, (rows, LANES), 1) < HEAD_DIM
    a, b = (
        jnp.broadcast_to(columns[:, first + 2 * h + j : first + 2 * h + j + 1], (rows, LANES))
        for j in range(2)
    )
    return jnp.where(left, a, b)


def head_row(values):
    lane = lax.broadcasted_iota(jnp.int32, (1, WIDE), 1)
    row = jnp.broadcast_to(values[0], (1, WIDE))
    for j in range(1, HEADS_AT_ONCE):
        row = jnp.where(lane >= j * HEAD_DIM, jnp.broadcast_to(values[j], (1, WIDE)), row)
    return row


def total_row(total):
    return head_row([total[j : j + 1] for j in range(HEADS_AT_ONCE)])


def scalar_row(values, chunk):
    return head_row([values[chunk * HEADS_AT_ONCE + j] for j in range(HEADS_AT_ONCE)])


def load_extended(ext, rim, body):
    for h in range(body.shape[1] // LANES):
        lanes = slice(h * LANES, (h + 1) * LANES)
        ext[h, 0:EDGE, :] = rim[RIM - EDGE :, lanes].astype(F32)
        ext[h, EDGE : EDGE + body.shape[0], :] = body[:, lanes].astype(F32)


def behind(ext, h, start, k):
    return ext[h, EDGE + start - k : EDGE + start - k + SUB, :]


def conv_rows(ext, taps, h, start):
    lanes = slice(h * LANES, (h + 1) * LANES)
    out = taps[0:1, lanes] * behind(ext, h, start, 0)
    for k in range(1, taps.shape[0]):
        out = out + taps[k : k + 1, lanes] * behind(ext, h, start, k)
    return out


def silu_parts(half):
    t = jnp.tanh(half)
    a = 1.0 + t
    silu = half * a
    return silu, a + silu * (1.0 - t)


def silu_of(half):
    return half + half * jnp.tanh(half)


def pieces(k):
    for s in range(0, GROUP, SUB):
        for h in range(HALVES):
            here = k * GROUP + s
            yield slice(here, here + SUB), slice(h * LANES, (h + 1) * LANES), slice(s, s + SUB), h


def head_picks():
    shape = (WIDE, LANES)
    return (
        lax.broadcasted_iota(jnp.int32, shape, 0) // HEAD_DIM
        == lax.broadcasted_iota(jnp.int32, shape, 1)
    ).astype(BF16)


def rows_of(k):
    return slice(k * GROUP, (k + 1) * GROUP)


def prep_kernel(rates, x, bcraw, dt, rim, steps_out, within_out):
    channels = x.shape[1]
    rim[:, :channels] = x[...]
    rim[:, channels:] = bcraw[...]
    length = dt.shape[1]
    row = lax.broadcasted_iota(jnp.int32, (2 * HEADS_AT_ONCE, length), 0)
    for c in range(steps_out.shape[0]):
        steps = dt[c * HEADS_AT_ONCE : (c + 1) * HEADS_AT_ONCE, :]
        steps = jnp.concatenate([steps, steps], axis=0)
        rate = jnp.zeros((2 * HEADS_AT_ONCE, length), F32)
        for j in range(HEADS_AT_ONCE):
            rate = jnp.where(row % HEADS_AT_ONCE == j, rates[c * HEADS_AT_ONCE + j], rate)
        steps_out[c] = steps
        within_out[c] = running_sum(rate * steps)


def gate_kernel(z, up, steps, within, d_out, dy_out, gz_out):
    for c in range(d_out.shape[0]):
        columns, _ = token_columns(within[c], steps[c], 0)
        for rows, lanes, part, h in pieces(0):
            here = slice(c * WIDE + lanes.start, c * WIDE + lanes.stop)
            silu, slope = silu_parts(0.5 * z[rows, here].astype(F32))
            upstream = up[rows, here].astype(F32)
            dy = (upstream * silu).astype(BF16)
            dy_out[c, rows, lanes] = dy
            gz_out[c, rows, lanes] = (upstream * slope).astype(BF16)
            v = over_lanes(columns[part], HEADS_AT_ONCE, h)
            d_out[c, rows, lanes] = (v * dy.astype(F32)).astype(BF16)


def gate_out_kernel(gate_base, gate_scale, bc, s_in, gate_out):
    n = s_in.shape[2]
    for c in range(gate_base.shape[0]):
        y1 = dot(bc[:, n:], s_in[c, 0])
        for rows, lanes, part, h in pieces(0):
            here = slice(c * WIDE + lanes.start, c * WIDE + lanes.stop)
            gate_out[rows, here] = (
                gate_base[c, rows, lanes].astype(F32)
                + gate_scale[c, rows, lanes].astype(F32) * y1[part, lanes]
            ).astype(BF16)


def first_kernel(
    count, place, rim_x, rim_bc, x, bcraw, steps, within, taps, bc_taps, d,
    w_out, bc_out, lower, upper, states, grads, *rest,
):
    sends = rest[: count - 1]
    ext, bc_ext, bct, ctd = rest[count - 1 :]
    length = x.shape[0]
    blocks = length // GROUP
    n = bcraw.shape[1] // 2

    @pl.when(pl.program_id(0) == 0)
    def _():
        load_extended(bc_ext, rim_bc, bcraw)
        bc_half = 0.5 * bc_taps[...]
        r = lax.broadcasted_iota(jnp.int32, (GROUP, GROUP), 0)
        c = lax.broadcasted_iota(jnp.int32, (GROUP, GROUP), 1)
        for k in range(blocks):
            for rows, lanes, part, h in pieces(k):
                post = silu_of(conv_rows(bc_ext, bc_half, h, rows.start)).astype(BF16)
                bc_out[rows, lanes] = post
                bct[k, lanes, part] = post.astype(F32).T.astype(BF16)
            b, cc = bc_out[rows_of(k), :n], bc_out[rows_of(k), n:]
            lower[k] = jnp.where(r >= c, dot(cc, bct[k, :n, :]), 0.0).astype(BF16)
            upper[k] = jnp.where(r <= c, dot(b, bct[k, n:, :]), 0.0).astype(BF16)

    load_extended(ext, rim_x, x)
    half_taps = 0.5 * taps[...]
    state = jnp.zeros((n, WIDE), F32)
    totals = []
    for k in range(blocks):
        columns, total = token_columns(within, steps, k)
        for rows, lanes, part, h in pieces(k):
            post = silu_of(conv_rows(ext, half_taps, h, rows.start)).astype(BF16).astype(F32)
            w_out[rows, lanes] = (over_lanes(columns[part], 0, h) * post).astype(BF16)
        total = total_row(total)
        totals.append(total)
        states[k] = state.astype(BF16)
        half = jnp.exp(-0.5 * total)
        state = jnp.exp(-total) * state + half * dot(bct[k, :n, :], w_out[rows_of(k), :])
        ctd[k] = half * dot(bct[k, n:, :], d[rows_of(k), :])
    grad = jnp.zeros((n, WIDE), F32)
    for k in reversed(range(blocks)):
        grads[k] = grad.astype(BF16)
        grad = jnp.exp(-totals[k]) * grad + ctd[k]
    whole = sum(totals[1:], totals[0])
    high = whole.astype(BF16).astype(F32)
    mid = (whole - high).astype(BF16).astype(F32)
    low = whole - high - mid
    r = lax.broadcasted_iota(jnp.int32, (RIM, WIDE), 0)
    extra = jnp.where(r == 0, high, jnp.where(r == 1, mid, jnp.where(r == 2, low, 0.0))).astype(BF16)
    for k in range(1, count):
        onward = place[0] + k < count
        sends[k - 1][0:n, :] = jnp.where(onward, state, grad).astype(BF16)
        sends[k - 1][n:, :] = extra


def inner_kernel(
    skips, rim_x, rim_bc, x, bcraw, dy, gz, steps, within, taps, bc_taps, w, d, bc, lower, upper,
    gate_base, gate_scale, slope_base, slope_scale, post_out, step_out, bc_part, bc_slope,
    ext, bc_ext, mix, quick,
):
    blocks = x.shape[0] // GROUP
    n = bc.shape[1] // 2
    chunk = pl.program_id(0)

    @pl.when(chunk == 0)
    def _():
        mix[...] = jnp.zeros_like(mix)

    load_extended(ext, rim_x, x)
    half_taps = 0.5 * taps[...]
    half_skip = 0.5 * scalar_row(skips, chunk)
    picks = head_picks()
    for k in range(blocks):
        columns, _ = token_columns(within, steps, k)
        columns = 0.5 * columns
        y0 = dot(lower[k], w[rows_of(k), :])
        p0 = dot(upper[k], d[rows_of(k), :])
        mix[k] += dot_t(d[rows_of(k), :], w[rows_of(k), :])
        for rows, lanes, part, h in pieces(k):
            silu, slope = silu_parts(conv_rows(ext, half_taps, h, rows.start))
            post_b = silu.astype(BF16)
            post = post_b.astype(F32)
            post_out[rows, lanes] = post_b
            skip = half_skip[:, lanes]
            v = over_lanes(columns[part], HEADS_AT_ONCE, h)
            gate = gz[rows, lanes].astype(F32)
            gate_base[rows, lanes] = (gate * (v * y0[part, lanes] + skip * post)).astype(BF16)
            gate_scale[rows, lanes] = (gate * v).astype(BF16)
            ud = over_lanes(columns[part], 0, h)
            p = p0[part, lanes]
            slope_base[rows, lanes] = (
                slope * (ud * p + skip * dy[rows, lanes].astype(F32))
            ).astype(BF16)
            slope_scale[rows, lanes] = (slope * ud).astype(BF16)
            quick[part, lanes] = (post * p).astype(BF16)
        step_out[:, rows_of(k)] = dot(quick[...], picks).T[: 2 * HEADS_AT_ONCE]

    @pl.when(chunk == pl.num_programs(0) - 1)
    def _():
        load_extended(bc_ext, rim_bc, bcraw)
        bc_half = 0.5 * bc_taps[...]
        r = lax.broadcasted_iota(jnp.int32, (GROUP, GROUP), 0)
        c = lax.broadcasted_iota(jnp.int32, (GROUP, GROUP), 1)
        for k in range(blocks):
            m = jnp.where(r >= c, mix[k], 0.0)
            bc_part[rows_of(k), n:] = dot(m.astype(BF16), bc[rows_of(k), :n])
            bc_part[rows_of(k), :n] = dot(m.T.astype(BF16), bc[rows_of(k), n:])
            for rows, lanes, part, h in pieces(k):
                bc_slope[rows, lanes] = 0.5 * silu_parts(conv_rows(bc_ext, bc_half, h, rows.start))[1]


def shared_kernel(
    count, shares, tap_count, place, rim_bc, bcraw, bc_slope, within, w, d, states, grads, bc_part,
    bc, slope_base, slope_scale, *rest,
):
    gets = rest[: count - 1]
    s_out, g_out, own, own_slope, sent, head_rows, acc, bc_ext = rest[count - 1 :]
    length = w.shape[0]
    blocks = length // GROUP
    n = bcraw.shape[1] // 2
    chunk = pl.program_id(0)

    @pl.when(chunk == 0)
    def _():
        acc[...] = bc_part[...]

    state_in = jnp.zeros((n, WIDE), F32)
    grad_in = jnp.zeros((n, WIDE), F32)
    spans = [None] + [
        sum(get[n + j : n + j + 1, :].astype(F32) for j in range(3)) for get in gets
    ]
    gone = jnp.zeros((1, WIDE), F32)
    for k in range(1, count):
        weight = jnp.where(place[0] >= k, jnp.exp(-gone), 0.0)
        state_in = state_in + weight * gets[k - 1][0:n, :].astype(F32)
        gone = gone + spans[k]
    gone = jnp.zeros((1, WIDE), F32)
    for ahead in range(1, count):
        k = count - ahead
        weight = jnp.where(place[0] < k, jnp.exp(-gone), 0.0)
        grad_in = grad_in + weight * gets[k - 1][0:n, :].astype(F32)
        gone = gone + spans[k]
    totals = [
        total_row(within[:, (k + 1) * GROUP - 1 : (k + 1) * GROUP]) for k in range(blocks)
    ]
    gone = jnp.zeros((1, WIDE), F32)
    for k in range(blocks):
        half = jnp.exp(-0.5 * totals[k])
        later = sum(totals[k + 1 :], jnp.zeros((1, WIDE), F32))
        sk = (half * (states[k].astype(F32) + jnp.exp(-gone) * state_in)).astype(BF16)
        gk = (half * (grads[k].astype(F32) + jnp.exp(-later) * grad_in)).astype(BF16)
        gone = gone + totals[k]
        s_out[k] = sk
        g_out[k] = gk
        if k == 0:
            p = dot(bc[...], gk)[0:EDGE]
            head_rows[...] = (
                slope_base[0:EDGE, :].astype(F32) + slope_scale[0:EDGE, :].astype(F32) * p
            )
        acc[rows_of(k), n:] += dot_t(d[rows_of(k), :], sk)
        acc[rows_of(k), :n] += dot_t(w[rows_of(k), :], gk)

    @pl.when(chunk == pl.num_programs(0) - 1)
    def _():
        load_extended(bc_ext, rim_bc, bcraw)
        share = length // shares
        taps = tap_count
        sums = {}
        for k in range(blocks):
            for rows, lanes, part, h in pieces(k):
                full = bc_slope[rows, lanes] * acc[rows, lanes]
                for j in range(taps):
                    fresh = jnp.sum(
                        (full * behind(bc_ext, h, rows.start, j)).reshape(SUB // 8, 8, LANES), axis=0
                    )
                    sums[h, j] = sums[h, j] + fresh if (h, j) in sums else fresh
        halves = []
        for h in range(HALVES):
            halves.append([jnp.sum(sums[h, j], axis=0, keepdims=True) for j in range(taps)])
        rows = shares // 2 * share
        own[rows:, :] = jnp.zeros((RIM, 2 * n), F32)
        for j in range(taps):
            for h in range(HALVES):
                own[rows + j : rows + j + 1, h * LANES : (h + 1) * LANES] = halves[h][j]
        sent[rows:, :] = split_rows(own[rows:, :])
        own[rows:, :] = joined_rows(split_rows(own[rows:, :]))
        core = lax.rem(place[1], 2)
        own_slope[...] = bc_slope[pl.ds(pl.multiple_of(place[1] * share, share), share), :]
        for j in range(shares // 2):
            here = slice(j * share, (j + 1) * share)
            start = pl.multiple_of((2 * j + core) * share, share)
            own[here, :] = acc[pl.ds(start, share), :]
            start = pl.multiple_of((2 * j + 1 - core) * share, share)
            sent[here, :] = acc[pl.ds(start, share), :].astype(BF16)


def split_rows(rows):
    high = rows.astype(BF16).astype(F32)
    return (high + pltpu.roll(rows - high, RIM // 2, axis=0)).astype(BF16)


def joined_rows(rows):
    rows = rows.astype(F32)
    return rows + pltpu.roll(rows, RIM // 2, axis=0)


def merge_kernel(place, own, get, mine, *sends):
    share = mine.shape[0] - RIM
    rows = own.shape[0] - RIM
    far_place = lax.div(place[1], 2)
    place_rows = lax.broadcasted_iota(jnp.int32, (RIM, own.shape[1]), 0)
    taps = own[rows:, :] + joined_rows(get[rows:, :])
    packed = split_rows(jnp.where(place_rows < RIM // 2, taps, 0.0))
    start = pl.multiple_of(far_place * share, share)
    mine[0:share, :] = own[pl.ds(start, share), :] + get[pl.ds(start, share), :].astype(F32)
    mine[share:, :] = joined_rows(packed)
    for j in range(1, len(sends) + 1):
        start = pl.multiple_of(lax.bitwise_xor(far_place, jnp.int32(j)) * share, share)
        total = own[pl.ds(start, share), :] + get[pl.ds(start, share), :].astype(F32)
        sends[j - 1][0:share, :] = total.astype(BF16)
        sends[j - 1][share:, :] = packed


def outer_kernel(
    rim_x, x, within, taps, slope_base, slope_scale, post, step_part, bc, g_in, x_next, after,
    x_out, step_out, tap_part, ext, slope_ext, quick,
):
    length = x.shape[0]
    blocks = length // GROUP
    load_extended(ext, rim_x, x)
    picks = head_picks()
    count = taps.shape[0]
    sums = {}
    for h in range(HALVES):
        slope_ext[h, length : length + EDGE, :] = x_next[:, h * LANES : (h + 1) * LANES]
    for k in range(blocks):
        p1 = dot(bc[rows_of(k), :], g_in[k])
        for rows, lanes, part, h in pieces(k):
            p = p1[part, lanes]
            slope = slope_base[rows, lanes].astype(F32) + slope_scale[rows, lanes].astype(F32) * p
            slope_ext[h, rows, :] = slope
            for j in range(count):
                fresh = jnp.sum(
                    (slope * behind(ext, h, rows.start, j)).reshape(SUB // 8, 8, LANES), axis=0
                )
                sums[h, j] = sums[h, j] + fresh if (h, j) in sums else fresh
            quick[part, lanes] = (post[rows, lanes].astype(F32) * p).astype(BF16)
        st = dot(quick[...], picks).T[: 2 * HEADS_AT_ONCE]
        step_out[:, rows_of(k)] = jnp.exp(token_gaps(within, k)[0]) * (st + step_part[:, rows_of(k)])
    for h in range(HALVES):
        lanes = slice(h * LANES, (h + 1) * LANES)
        for j in range(count):
            tap_part[j : j + 1, lanes] = jnp.sum(sums[h, j], axis=0, keepdims=True)
        for s in range(0, length, SUB):
            out = taps[0:1, lanes] * slope_ext[h, s : s + SUB, :]
            for j in range(1, count):
                out = out + taps[j : j + 1, lanes] * slope_ext[h, s + j : s + j + SUB, :]
            x_out[s : s + SUB, lanes] = out.astype(BF16)


def last_kernel(own, own_slope, *rest):
    gets, rows_out, taps_out = rest[:-2], rest[-2], rest[-1]
    share = own_slope.shape[0]
    parts = [own[...]] + [
        jnp.concatenate([get[0:share, :].astype(F32), joined_rows(get[share:, :])], 0)
        for get in gets
    ]
    total = tree_sum(parts)
    rows_out[...] = total[0:share] * own_slope[...]
    taps_out[...] = total[share : share + taps_out.shape[0]]


def local(xraw, zgate, bcraw, dt, a_rate, d_skip, conv_x, conv_bc, dout):
    length, channels = xraw.shape
    heads = a_rate.shape[0]
    n2 = bcraw.shape[1]
    n = n2 // 2
    taps = conv_x.shape[0]
    blocks = length // GROUP
    chunks = channels // WIDE
    count = lax.axis_size("seq")
    shares = lax.axis_size("head")
    share = length // shares
    place = jnp.stack([lax.axis_index("seq"), lax.axis_index("head")]).astype(jnp.int32)

    tall = pl.BlockSpec((length, WIDE), lambda c: (0, c))
    slab = pl.BlockSpec((None, length, WIDE), lambda c: (c, 0, 0))
    top = pl.BlockSpec((None, RIM, WIDE), lambda c: (c, 0, 0))
    band = pl.BlockSpec((GROUP, channels), lambda k: (k, 0))
    band_slab = pl.BlockSpec((chunks, GROUP, WIDE), lambda k: (0, k, 0))
    band_pair = pl.BlockSpec((chunks, 2 * HEADS_AT_ONCE, GROUP), lambda k: (0, 0, k))
    edge = pl.BlockSpec((EDGE, WIDE), lambda c: (0, c))
    rim = pl.BlockSpec((RIM, WIDE), lambda c: (0, c))
    bc_rim = pl.BlockSpec((RIM, n2), lambda c: (0, channels // n2))
    tap = pl.BlockSpec((taps, WIDE), lambda c: (0, c))
    pair = pl.BlockSpec((None, 2 * HEADS_AT_ONCE, length), lambda c: (c, 0, 0))
    state = pl.BlockSpec((None, blocks, n, WIDE), lambda c: (c, 0, 0, 0))
    carry = pl.BlockSpec((None, n + RIM, WIDE), lambda c: (c, 0, 0))
    scalar = pl.BlockSpec(memory_space=pltpu.SMEM)

    def fixed(*shape):
        return pl.BlockSpec(shape, lambda c: (0,) * len(shape))

    def arr(shape, dtype):
        return jax.ShapeDtypeStruct(shape, dtype)

    def far(value):
        return pltpu.with_memory_space_constraint(value, pltpu.HBM)

    def near(value):
        return pltpu.with_memory_space_constraint(value, pltpu.VMEM)

    params = pltpu.CompilerParams(
        dimension_semantics=("arbitrary",), vmem_limit_bytes=32 * 1024 * 1024
    )
    cover = pl.CostEstimate(
        flops=40_000_000_000, transcendentals=0, bytes_accessed=30_000_000
    )
    ext_x = pltpu.VMEM((HALVES, length + EDGE, LANES), F32)
    ext_bc = pltpu.VMEM((n2 // LANES, length + EDGE, LANES), F32)
    final = arr((length, channels), BF16)
    wide = pltpu.VMEM((chunks, length, WIDE), BF16)
    square = (blocks, GROUP, GROUP)
    stack = pltpu.VMEM((chunks, blocks, n, WIDE), BF16)
    xraw, zgate, dout, dt, bcraw, taps_x, taps_bc = (
        far(v) for v in (xraw, zgate, dout, dt, bcraw, conv_x, conv_bc)
    )
    pairs = arr((chunks, 2 * HEADS_AT_ONCE, length), F32)

    last = length // RIM - 1
    rim_rows, steps, within = pl.pallas_call(
        prep_kernel,
        grid=(1,),
        in_specs=[scalar, pl.BlockSpec((RIM, channels), lambda c: (last, 0)),
                  pl.BlockSpec((RIM, n2), lambda c: (last, 0)), fixed(heads, length)],
        out_specs=[fixed(RIM, channels + n2), fixed(*pairs.shape), fixed(*pairs.shape)],
        out_shape=[arr((RIM, channels + n2), BF16), pairs, pairs],
        compiler_params=params,
        name="prep",
    )(a_rate, xraw, bcraw, dt)
    before = from_behind(rim_rows, "seq", 1)
    gated = pl.pallas_call(
        gate_kernel,
        grid=(blocks,),
        in_specs=[band, band, band_pair, band_pair],
        out_specs=[band_slab] * 3,
        out_shape=[wide] * 3,
        compiler_params=params,
        cost_estimate=cover,
        name="gate",
    )(zgate, dout, steps, within)

    d, dy, gz = map(near, gated)
    first = pl.pallas_call(
        functools.partial(first_kernel, count),
        grid=(chunks,),
        in_specs=[scalar, rim, bc_rim, tall, fixed(length, n2), pair, pair, tap, fixed(taps, n2),
                  slab],
        out_specs=[slab, fixed(length, n2), fixed(*square), fixed(*square), state, state]
        + [carry] * (count - 1),
        out_shape=[wide, arr((length, n2), BF16), arr(square, BF16), arr(square, BF16),
                   stack, stack] + [arr((chunks, n + RIM, WIDE), BF16)] * (count - 1),
        scratch_shapes=[ext_x, ext_bc, pltpu.VMEM((blocks, n2, GROUP), BF16),
                        pltpu.VMEM((blocks, n, WIDE), F32)],
        compiler_params=params,
        name="first",
    )(place, before, before, xraw, bcraw, steps, within, taps_x, taps_bc, d)
    w, bc, lower, upper, states, grads = first[:6]
    w, states, grads = map(near, (w, states, grads))
    gets = [shifted(sent, "seq", k + 1) for k, sent in enumerate(first[6:])]

    inner = pl.pallas_call(
        inner_kernel,
        grid=(chunks,),
        in_specs=[scalar, rim, bc_rim, tall, fixed(length, n2), slab, slab, pair, pair, tap,
                  fixed(taps, n2), slab, slab, fixed(length, n2), fixed(*square), fixed(*square)],
        out_specs=[slab] * 5 + [pair, fixed(length, n2), fixed(length, n2)],
        out_shape=[wide] * 5 + [pairs, arr((length, n2), F32), arr((length, n2), F32)],
        scratch_shapes=[ext_x, ext_bc, pltpu.VMEM(square, F32), pltpu.VMEM((GROUP, WIDE), BF16)],
        compiler_params=params,
        cost_estimate=cover,
        name="inner",
    )(d_skip, before, before, xraw, bcraw, dy, gz, steps, within, taps_x, taps_bc, w, d, bc,
      lower, upper)
    gate_base, gate_scale, slope_base, slope_scale, post = map(near, inner[:5])
    step_part, bc_part, bc_slope = inner[5:]

    half = shares // 2 * share + RIM
    shared = pl.pallas_call(
        functools.partial(shared_kernel, count, shares, taps),
        grid=(chunks,),
        in_specs=[scalar, bc_rim, fixed(length, n2), fixed(length, n2), pair, slab, slab, state,
                  state, fixed(length, n2), fixed(RIM, n), top, top] + [carry] * (count - 1),
        out_specs=[state, state, fixed(half, n2), fixed(share, n2), fixed(half, n2), edge],
        out_shape=[stack, stack, arr((half, n2), F32), arr((share, n2), F32),
                   arr((half, n2), BF16), arr((EDGE, channels), F32)],
        scratch_shapes=[pltpu.VMEM((length, n2), F32), ext_bc],
        compiler_params=params,
        name="shared",
    )(place, before, bcraw, bc_slope, within, w, d, states, grads, bc_part, bc, slope_base,
      slope_scale, *gets)
    s_in, g_in, own, own_slope, sent, head_rows = shared
    s_in, g_in = near(s_in), near(g_in)
    x_next = from_behind(head_rows, "seq", -1)
    got = swapped(sent, "head", 1)

    gate_grad = pl.pallas_call(
        gate_out_kernel,
        grid=(blocks,),
        in_specs=[band_slab, band_slab, pl.BlockSpec((GROUP, n2), lambda k: (k, 0)),
                  pl.BlockSpec((chunks, 1, n, WIDE), lambda k: (0, k, 0, 0))],
        out_specs=band,
        out_shape=final,
        compiler_params=params,
        cost_estimate=cover,
        name="gate_out",
    )(gate_base, gate_scale, bc, s_in)

    merged = pl.pallas_call(
        merge_kernel,
        grid=(1,),
        in_specs=[scalar, fixed(half, n2), fixed(half, n2)],
        out_specs=[fixed(share + RIM, n2)] * (shares // 2),
        out_shape=[arr((share + RIM, n2), F32)]
        + [arr((share + RIM, n2), BF16)] * (shares // 2 - 1),
        compiler_params=params,
        name="merge",
    )(place, own, got)
    own_parts = [swapped(part, "head", 2 * j + 2) for j, part in enumerate(merged[1:])]

    outer = pl.pallas_call(
        outer_kernel,
        grid=(chunks,),
        in_specs=[rim, tall, pair, tap, slab, slab, slab, pair, fixed(length, n), state, edge,
                  pl.BlockSpec(memory_space=pl.ANY)],
        out_specs=[tall, pair, tap],
        out_shape=[final, pairs, arr((taps, channels), F32)],
        scratch_shapes=[ext_x, ext_x, pltpu.VMEM((GROUP, WIDE), BF16)],
        compiler_params=params,
        cost_estimate=cover,
        name="outer",
    )(before, xraw, within, taps_x, slope_base, slope_scale, post, step_part, bc, g_in, x_next,
      merged[0])
    x_raw_grad, step_pairs, x_taps_part = outer

    own_rows, bc_taps_part = pl.pallas_call(
        last_kernel,
        grid=(1,),
        in_specs=[fixed(share + RIM, n2), fixed(share, n2)]
        + [fixed(share + RIM, n2)] * (shares // 2 - 1),
        out_specs=[fixed(share, n2), fixed(taps, n2)],
        out_shape=[arr((share, n2), F32), arr((taps, n2), F32)],
        compiler_params=params,
        name="last",
    )(merged[0], own_slope, *own_parts)

    step_grad = step_pairs[:, :HEADS_AT_ONCE].reshape(heads, length)
    next_rows = from_behind(own_rows[:EDGE], ("seq", "head"), -1)
    own_ext = jnp.concatenate([own_rows, next_rows], axis=0)
    bc_raw_grad = sum(conv_bc[k][None] * own_ext[k : k + share] for k in range(taps))
    tap_sums = sum_over(jnp.concatenate([x_taps_part, bc_taps_part], axis=1), "seq")
    return (x_raw_grad, gate_grad, step_grad, bc_raw_grad, tap_sums[:, :channels],
            tap_sums[:, channels:])


def solution(mesh):
    placed = (
        P("seq", "head"),
        P("seq", "head"),
        P("seq", None),
        P("head", "seq"),
        P("head"),
        P("head"),
        P(None, "head"),
        P(),
        P("seq", "head"),
    )
    return jax.shard_map(
        local,
        mesh=mesh,
        in_specs=placed,
        out_specs=(
            P("seq", "head"),
            P("seq", "head"),
            P("head", "seq"),
            P(("seq", "head"), None),
            P(None, "head"),
            P(),
        ),
        check_vma=False,
    )
```

```python
import functools

import jax
import jax.numpy as jnp
from jax import lax
from jax.experimental import pallas as pl
from jax.experimental.pallas import tpu as pltpu
from jax.sharding import PartitionSpec as P

HEAD_DIM = 64
GROUP = 256
HEADS_AT_ONCE = 4
WIDE = HEAD_DIM * HEADS_AT_ONCE
LANES = 2 * HEAD_DIM
HALVES = HEADS_AT_ONCE // 2
SUB = 128
EDGE = 8
RIM = 16
F32 = jnp.float32
BF16 = jnp.bfloat16


def shifted(value, axis, steps):
    count = lax.axis_size(axis)
    return lax.ppermute(value, axis, [(i, (i + steps) % count) for i in range(count)])


def from_behind(value, axis, steps):
    count = lax.axis_size(axis)
    first, last = (max(0, -steps), min(count, count - steps))
    return lax.ppermute(value, axis, [(i, i + steps) for i in range(first, last)])


def swapped(value, axis, k):
    return lax.ppermute(value, axis, [(i, i ^ k) for i in range(lax.axis_size(axis))])


def tree_sum(parts):
    while len(parts) > 1:
        parts = [a + b for a, b in zip(parts[::2], parts[1::2])]
    return parts[0]


def sum_over(value, axis):
    k = 1
    while 2 * k < lax.axis_size(axis):
        value = value + swapped(value, axis, k)
        k *= 2
    return value, swapped(value, axis, k)


def dot(a, b):
    return jnp.dot(a, b, preferred_element_type=F32)


def dot_t(a, b):
    return lax.dot_general(a, b, (((1,), (1,)), ((), ())), preferred_element_type=F32)


def running_sum(g):
    place = lax.broadcasted_iota(jnp.int32, g.shape, 1) % GROUP
    step = 1
    while step < GROUP:
        g = g + jnp.where(place >= step, pltpu.roll(g, step, axis=1), 0.0)
        step *= 2
    return g


def token_gaps(within, k):
    w = within[:, rows_of(k)]
    total = w[:, GROUP - 1 : GROUP]
    return w - 0.5 * total, total


def token_columns(within, steps, k):
    gap, _ = token_gaps(within, k)
    upper = lax.broadcasted_iota(jnp.int32, gap.shape, 0) < HEADS_AT_ONCE
    e = jnp.exp(jnp.where(upper, gap, -gap))
    return jnp.where(upper, e * steps[:, rows_of(k)], e).T


def over_lanes(columns, first, h):
    rows = columns.shape[0]
    left = lax.broadcasted_iota(jnp.int32, (rows, LANES), 1) < HEAD_DIM
    a, b = (
        jnp.broadcast_to(columns[:, first + 2 * h + j : first + 2 * h + j + 1], (rows, LANES))
        for j in range(2)
    )
    return jnp.where(left, a, b)


def head_row(values):
    lane = lax.broadcasted_iota(jnp.int32, (1, WIDE), 1)
    row = jnp.broadcast_to(values[0], (1, WIDE))
    for j in range(1, HEADS_AT_ONCE):
        row = jnp.where(lane >= j * HEAD_DIM, jnp.broadcast_to(values[j], (1, WIDE)), row)
    return row


def total_row(total):
    return head_row([total[j : j + 1] for j in range(HEADS_AT_ONCE)])


def scalar_row(values, chunk):
    return head_row([values[chunk * HEADS_AT_ONCE + j] for j in range(HEADS_AT_ONCE)])


def load_extended(ext, rim, body):
    for h in range(body.shape[1] // LANES):
        lanes = slice(h * LANES, (h + 1) * LANES)
        ext[h, 0:EDGE, :] = rim[RIM - EDGE :, lanes].astype(F32)
        ext[h, EDGE : EDGE + body.shape[0], :] = body[:, lanes].astype(F32)


def behind(ext, h, start, k):
    return ext[h, EDGE + start - k : EDGE + start - k + SUB, :]


def conv_rows(ext, taps, h, start):
    lanes = slice(h * LANES, (h + 1) * LANES)
    out = taps[0:1, lanes] * behind(ext, h, start, 0)
    for k in range(1, taps.shape[0]):
        out = out + taps[k : k + 1, lanes] * behind(ext, h, start, k)
    return out


def silu_parts(half):
    t = jnp.tanh(half)
    a = 1.0 + t
    silu = half * a
    return silu, a + silu * (1.0 - t)


def silu_of(half):
    return half + half * jnp.tanh(half)


def pieces(k):
    for s in range(0, GROUP, SUB):
        for h in range(HALVES):
            here = k * GROUP + s
            yield slice(here, here + SUB), slice(h * LANES, (h + 1) * LANES), slice(s, s + SUB), h


def head_picks():
    shape = (WIDE, LANES)
    return (
        lax.broadcasted_iota(jnp.int32, shape, 0) // HEAD_DIM
        == lax.broadcasted_iota(jnp.int32, shape, 1)
    ).astype(BF16)


def chunk_lanes(c):
    return pl.ds(pl.multiple_of(c * WIDE, WIDE), WIDE)


def rows_of(k):
    if isinstance(k, int):
        return slice(k * GROUP, (k + 1) * GROUP)
    return pl.ds(pl.multiple_of(k * GROUP, GROUP), GROUP)


def prep_kernel(rates, x, bcraw, dt, rim, steps_out, within_out):
    channels = x.shape[1]
    rim[:, :channels] = x[...]
    rim[:, channels:] = bcraw[...]
    length = dt.shape[1]
    row = lax.broadcasted_iota(jnp.int32, (2 * HEADS_AT_ONCE, length), 0)
    for c in range(steps_out.shape[0]):
        steps = dt[c * HEADS_AT_ONCE : (c + 1) * HEADS_AT_ONCE, :]
        steps = jnp.concatenate([steps, steps], axis=0)
        rate = jnp.zeros((2 * HEADS_AT_ONCE, length), F32)
        for j in range(HEADS_AT_ONCE):
            rate = jnp.where(row % HEADS_AT_ONCE == j, rates[c * HEADS_AT_ONCE + j], rate)
        steps_out[c] = steps
        within_out[c] = running_sum(rate * steps)


def gate_kernel(
    x, z, up, steps, within, x_out, d_out, dy_out, gz_out, columns_out, z_buf, up_buf, sems
):
    chunks = d_out.shape[0]
    blocks = z_buf.shape[0]

    def copy(j, k):
        source, target = ((z, z_buf.at[k]), (up, up_buf.at[k]), (x, x_out.at[rows_of(k), :]))[j]
        return pltpu.make_async_copy(source.at[rows_of(k), :], target, sems.at[j, k])

    for k in range(blocks):
        copy(0, k).start()
        copy(1, k).start()
    for k in range(blocks):
        copy(2, k).start()

    @pl.loop(0, blocks)
    def _(k):
        copy(0, k).wait()
        copy(1, k).wait()
        for c in range(chunks):
            columns = token_columns(within.at[c], steps.at[c], k)
            columns_out[c, rows_of(k), :] = columns
            for part_rows, lanes, part, h in pieces(0):
                here = slice(c * WIDE + lanes.start, c * WIDE + lanes.stop)
                rows = pl.ds(pl.multiple_of(k * GROUP + part.start, SUB), SUB)
                silu, slope = silu_parts(0.5 * z_buf[k, part, here].astype(F32))
                upstream = up_buf[k, part, here].astype(F32)
                dy = (upstream * silu).astype(BF16)
                dy_out[c, rows, lanes] = dy
                gz_out[c, rows, lanes] = (upstream * slope).astype(BF16)
                v = over_lanes(columns[part], HEADS_AT_ONCE, h)
                d_out[c, rows, lanes] = (v * dy.astype(F32)).astype(BF16)

    for k in range(blocks):
        copy(2, k).wait()


def gate_out_kernel(gate_base, gate_scale, bc, s_in, gate_out, buf, sems):
    chunks = buf.shape[0]
    n = s_in.shape[2]

    def copy(c):
        return pltpu.make_async_copy(buf.at[c], gate_out.at[:, chunk_lanes(c)], sems.at[c])

    @pl.loop(0, chunks)
    def _(c):
        for k in range(bc.shape[0] // GROUP):
            y1 = dot(bc[rows_of(k), n:], s_in[c, k])
            for rows, lanes, part, h in pieces(k):
                buf[c, rows, lanes] = (
                    gate_base[c, rows, lanes].astype(F32)
                    + gate_scale[c, rows, lanes].astype(F32) * y1[part, lanes]
                ).astype(BF16)
        copy(c).start()

    for c in range(chunks):
        copy(c).wait()


def first_kernel(
    count, place, rims, x_all, bcraw, columns_all, within_all, taps, bc_taps, d_all,
    w_all, bc_out, lower, upper, states_all, grads_all, *rest,
):
    sends_all = rest[: count - 1]
    ext, bc_ext, bct, ctd = rest[count - 1 :]
    length = bcraw.shape[0]
    blocks = length // GROUP
    n = bcraw.shape[1] // 2
    channels = taps.shape[1]

    load_extended(bc_ext, rims.at[:, channels:], bcraw)
    bc_half = 0.5 * bc_taps[...]
    r = lax.broadcasted_iota(jnp.int32, (GROUP, GROUP), 0)
    c = lax.broadcasted_iota(jnp.int32, (GROUP, GROUP), 1)
    for k in range(blocks):
        for rows, lanes, part, h in pieces(k):
            post = silu_of(conv_rows(bc_ext, bc_half, h, rows.start)).astype(BF16)
            bc_out[rows, lanes] = post
            bct[k, lanes, part] = post.astype(F32).T.astype(BF16)
        b, cc = bc_out[rows_of(k), :n], bc_out[rows_of(k), n:]
        lower[k] = jnp.where(r >= c, dot(cc, bct[k, :n, :]), 0.0).astype(BF16)
        upper[k] = jnp.where(r <= c, dot(b, bct[k, n:, :]), 0.0).astype(BF16)

    @pl.loop(0, w_all.shape[0])
    def _(c):
        columns, within, d, w_out, states, grads = (
            ref.at[c] for ref in (columns_all, within_all, d_all, w_all, states_all, grads_all)
        )
        x = x_all.at[:, chunk_lanes(c)]
        sends = [ref.at[c] for ref in sends_all]
        load_extended(ext, rims.at[:, chunk_lanes(c)], x)
        half_taps = 0.5 * taps[:, chunk_lanes(c)]
        state = jnp.zeros((n, WIDE), F32)
        totals = []
        for k in range(blocks):
            _, total = token_gaps(within, k)
            for rows, lanes, part, h in pieces(k):
                post = silu_of(conv_rows(ext, half_taps, h, rows.start)).astype(BF16).astype(F32)
                w_out[rows, lanes] = (over_lanes(columns[rows, :], 0, h) * post).astype(BF16)
            total = total_row(total)
            totals.append(total)
            states[k] = state.astype(BF16)
            half = jnp.exp(-0.5 * total)
            state = jnp.exp(-total) * state + half * dot(bct[k, :n, :], w_out[rows_of(k), :])
            ctd[k] = half * dot(bct[k, n:, :], d[rows_of(k), :])
        grad = jnp.zeros((n, WIDE), F32)
        for k in reversed(range(blocks)):
            grads[k] = grad.astype(BF16)
            grad = jnp.exp(-totals[k]) * grad + ctd[k]
        whole = sum(totals[1:], totals[0])
        high = whole.astype(BF16).astype(F32)
        mid = (whole - high).astype(BF16).astype(F32)
        low = whole - high - mid
        r = lax.broadcasted_iota(jnp.int32, (RIM, WIDE), 0)
        extra = jnp.where(r == 0, high, jnp.where(r == 1, mid, jnp.where(r == 2, low, 0.0))).astype(BF16)
        for k in range(1, count):
            onward = place[0] + k < count
            sends[k - 1][0:n, :] = jnp.where(onward, state, grad).astype(BF16)
            sends[k - 1][n:, :] = extra


def inner_kernel(
    skips, rims, x_all, bcraw, taps, bc_taps, bc, lower, upper,
    dy_all, gz_all, columns_all, w_all, d_all,
    gate_base_all, gate_scale_all, slope_base_all, slope_scale_all, post_all, step_all,
    bc_part, bc_slope, ext, bc_ext, mix, quick,
):
    channels = taps.shape[1]
    blocks = bc.shape[0] // GROUP
    n = bc.shape[1] // 2
    mix[...] = jnp.zeros_like(mix)
    picks = head_picks()

    @pl.loop(0, w_all.shape[0])
    def _(c):
        dy, gz, columns, w, d = (
            ref.at[c] for ref in (dy_all, gz_all, columns_all, w_all, d_all)
        )
        x = x_all.at[:, chunk_lanes(c)]
        gate_base, gate_scale, slope_base, slope_scale, post_out, step_out = (
            ref.at[c]
            for ref in (gate_base_all, gate_scale_all, slope_base_all, slope_scale_all, post_all,
                        step_all)
        )
        load_extended(ext, rims.at[:, chunk_lanes(c)], x)
        half_taps = 0.5 * taps[:, chunk_lanes(c)]
        half_skip = 0.5 * scalar_row(skips, c)
        for k in range(blocks):
            y0 = dot(lower[k], w[rows_of(k), :])
            p0 = dot(upper[k], d[rows_of(k), :])
            mix[k] += dot_t(d[rows_of(k), :], w[rows_of(k), :])
            for rows, lanes, part, h in pieces(k):
                silu, slope = silu_parts(conv_rows(ext, half_taps, h, rows.start))
                post_b = silu.astype(BF16)
                post = post_b.astype(F32)
                post_out[rows, lanes] = post_b
                skip = half_skip[:, lanes]
                scales = 0.5 * columns[rows, :]
                v = over_lanes(scales, HEADS_AT_ONCE, h)
                gate = gz[rows, lanes].astype(F32)
                gate_base[rows, lanes] = (gate * (v * y0[part, lanes] + skip * post)).astype(BF16)
                gate_scale[rows, lanes] = (gate * v).astype(BF16)
                ud = over_lanes(scales, 0, h)
                p = p0[part, lanes]
                slope_base[rows, lanes] = (
                    slope * (ud * p + skip * dy[rows, lanes].astype(F32))
                ).astype(BF16)
                slope_scale[rows, lanes] = (slope * ud).astype(BF16)
                quick[part, lanes] = (post * p).astype(BF16)
            step_out[:, rows_of(k)] = dot(quick[...], picks).T[: 2 * HEADS_AT_ONCE]

    load_extended(bc_ext, rims.at[:, channels:], bcraw)
    bc_half = 0.5 * bc_taps[...]
    r = lax.broadcasted_iota(jnp.int32, (GROUP, GROUP), 0)
    c = lax.broadcasted_iota(jnp.int32, (GROUP, GROUP), 1)
    for k in range(blocks):
        m = jnp.where(r >= c, mix[k], 0.0)
        bc_part[rows_of(k), n:] = dot(m.astype(BF16), bc[rows_of(k), :n])
        bc_part[rows_of(k), :n] = dot(m.T.astype(BF16), bc[rows_of(k), n:])
        for rows, lanes, part, h in pieces(k):
            bc_slope[rows, lanes] = 0.5 * silu_parts(conv_rows(bc_ext, bc_half, h, rows.start))[1]


def shared_kernel(
    count, shares, tap_count, place, rims, bcraw, bc_slope, bc_part, bc,
    within_all, w_all, d_all, states_all, grads_all, slope_base_all, slope_scale_all, *rest,
):
    gets_all = rest[: count - 1]
    s_all, g_all, own, own_slope, sent, heads_all, acc, bc_ext = rest[count - 1 :]
    length = bc.shape[0]
    blocks = length // GROUP
    n = bcraw.shape[1] // 2
    channels = heads_all.shape[1]
    acc[...] = bc_part[...]

    @pl.loop(0, w_all.shape[0])
    def _(c):
        within, w, d, states, grads, slope_base, slope_scale, s_out, g_out = (
            ref.at[c]
            for ref in (within_all, w_all, d_all, states_all, grads_all, slope_base_all,
                        slope_scale_all, s_all, g_all)
        )
        gets = [ref.at[c] for ref in gets_all]
        state_in = jnp.zeros((n, WIDE), F32)
        grad_in = jnp.zeros((n, WIDE), F32)
        spans = [None] + [
            sum(get[n + j : n + j + 1, :].astype(F32) for j in range(3)) for get in gets
        ]
        gone = jnp.zeros((1, WIDE), F32)
        for k in range(1, count):
            weight = jnp.where(place[0] >= k, jnp.exp(-gone), 0.0)
            state_in = state_in + weight * gets[k - 1][0:n, :].astype(F32)
            gone = gone + spans[k]
        gone = jnp.zeros((1, WIDE), F32)
        for ahead in range(1, count):
            k = count - ahead
            weight = jnp.where(place[0] < k, jnp.exp(-gone), 0.0)
            grad_in = grad_in + weight * gets[k - 1][0:n, :].astype(F32)
            gone = gone + spans[k]
        totals = [
            total_row(within[:, (k + 1) * GROUP - 1 : (k + 1) * GROUP]) for k in range(blocks)
        ]
        gone = jnp.zeros((1, WIDE), F32)
        for k in range(blocks):
            half = jnp.exp(-0.5 * totals[k])
            later = sum(totals[k + 1 :], jnp.zeros((1, WIDE), F32))
            sk = (half * (states[k].astype(F32) + jnp.exp(-gone) * state_in)).astype(BF16)
            gk = (half * (grads[k].astype(F32) + jnp.exp(-later) * grad_in)).astype(BF16)
            gone = gone + totals[k]
            s_out[k] = sk
            g_out[k] = gk
            if k == 0:
                p = dot(bc[0:RIM, :n], gk)[0:EDGE]
                heads_all[:, chunk_lanes(c)] = (
                    slope_base[0:EDGE, :].astype(F32) + slope_scale[0:EDGE, :].astype(F32) * p
                )
            acc[rows_of(k), n:] += dot_t(d[rows_of(k), :], sk)
            acc[rows_of(k), :n] += dot_t(w[rows_of(k), :], gk)

    load_extended(bc_ext, rims.at[:, channels:], bcraw)
    share = length // shares
    taps = tap_count
    sums = {}
    for k in range(blocks):
        for rows, lanes, part, h in pieces(k):
            full = bc_slope[rows, lanes] * acc[rows, lanes]
            for j in range(taps):
                fresh = jnp.sum(
                    (full * behind(bc_ext, h, rows.start, j)).reshape(SUB // 8, 8, LANES), axis=0
                )
                sums[h, j] = sums[h, j] + fresh if (h, j) in sums else fresh
    halves = []
    for h in range(HALVES):
        halves.append([jnp.sum(sums[h, j], axis=0, keepdims=True) for j in range(taps)])
    rows = shares // 2 * share
    own[rows:, :] = jnp.zeros((RIM, 2 * n), F32)
    for j in range(taps):
        for h in range(HALVES):
            own[rows + j : rows + j + 1, h * LANES : (h + 1) * LANES] = halves[h][j]
    sent[rows:, :] = split_rows(own[rows:, :])
    own[rows:, :] = joined_rows(split_rows(own[rows:, :]))
    core = lax.rem(place[1], 2)
    own_slope[...] = bc_slope[pl.ds(pl.multiple_of(place[1] * share, share), share), :]
    for j in range(shares // 2):
        here = slice(j * share, (j + 1) * share)
        start = pl.multiple_of((2 * j + core) * share, share)
        own[here, :] = acc[pl.ds(start, share), :]
        start = pl.multiple_of((2 * j + 1 - core) * share, share)
        sent[here, :] = acc[pl.ds(start, share), :].astype(BF16)


def split_rows(rows):
    high = rows.astype(BF16).astype(F32)
    return (high + pltpu.roll(rows - high, RIM // 2, axis=0)).astype(BF16)


def joined_rows(rows):
    rows = rows.astype(F32)
    return rows + pltpu.roll(rows, RIM // 2, axis=0)


def merge_kernel(place, own, get, mine, *sends):
    share = mine.shape[0] - RIM
    rows = own.shape[0] - RIM
    far_place = lax.div(place[1], 2)
    place_rows = lax.broadcasted_iota(jnp.int32, (RIM, own.shape[1]), 0)
    taps = own[rows:, :] + joined_rows(get[rows:, :])
    packed = split_rows(jnp.where(place_rows < RIM // 2, taps, 0.0))
    start = pl.multiple_of(far_place * share, share)
    mine[0:share, :] = own[pl.ds(start, share), :] + get[pl.ds(start, share), :].astype(F32)
    mine[share:, :] = joined_rows(packed)
    for j in range(1, len(sends) + 1):
        start = pl.multiple_of(lax.bitwise_xor(far_place, jnp.int32(j)) * share, share)
        total = own[pl.ds(start, share), :] + get[pl.ds(start, share), :].astype(F32)
        sends[j - 1][0:share, :] = total.astype(BF16)
        sends[j - 1][share:, :] = packed


def outer_kernel(
    rims, taps_all, bc, x_next, after, x_all, within_all, slope_base_all, slope_scale_all, post_all,
    steps_all, g_all, x_out_all, step_out_all, tap_part, ext, slope_ext, quick, buf, step_buf, sems,
):
    length = bc.shape[0]
    blocks = length // GROUP
    n = g_all.shape[2]
    count = taps_all.shape[0]
    chunks = buf.shape[0]
    picks = head_picks()

    def copy(c):
        return pltpu.make_async_copy(buf.at[c], x_out_all.at[:, chunk_lanes(c)], sems.at[c])

    @pl.loop(0, chunks)
    def _(c):
        x = x_all.at[:, chunk_lanes(c)]
        within, slope_base, slope_scale, post, step_part, g_in, x_out, step_out = (
            ref.at[c]
            for ref in (within_all, slope_base_all, slope_scale_all, post_all, steps_all,
                        g_all, buf, step_buf)
        )
        load_extended(ext, rims.at[:, chunk_lanes(c)], x)
        taps = taps_all[:, chunk_lanes(c)]
        following = x_next[:, chunk_lanes(c)]
        sums = {}
        for h in range(HALVES):
            slope_ext[h, length : length + EDGE, :] = following[:, h * LANES : (h + 1) * LANES]
        for k in range(blocks):
            p1 = dot(bc[rows_of(k), :n], g_in[k])
            for rows, lanes, part, h in pieces(k):
                p = p1[part, lanes]
                slope = slope_base[rows, lanes].astype(F32) + slope_scale[rows, lanes].astype(F32) * p
                slope_ext[h, rows, :] = slope
                for j in range(count):
                    fresh = jnp.sum(
                        (slope * behind(ext, h, rows.start, j)).reshape(SUB // 8, 8, LANES), axis=0
                    )
                    sums[h, j] = sums[h, j] + fresh if (h, j) in sums else fresh
                quick[part, lanes] = (post[rows, lanes].astype(F32) * p).astype(BF16)
            st = dot(quick[...], picks).T[: 2 * HEADS_AT_ONCE]
            step_out[:, rows_of(k)] = jnp.exp(token_gaps(within, k)[0]) * (st + step_part[:, rows_of(k)])
        tap_part[:, chunk_lanes(c)] = jnp.concatenate(
            [
                jnp.concatenate(
                    [jnp.sum(sums[h, j], axis=0, keepdims=True) for h in range(HALVES)], axis=1
                )
                for j in range(count)
            ],
            axis=0,
        )
        for h in range(HALVES):
            lanes = slice(h * LANES, (h + 1) * LANES)
            for s in range(0, length, SUB):
                out = taps[0:1, lanes] * slope_ext[h, s : s + SUB, :]
                for j in range(1, count):
                    out = out + taps[j : j + 1, lanes] * slope_ext[h, s + j : s + j + SUB, :]
                x_out[s : s + SUB, lanes] = out.astype(BF16)
        copy(c).start()

    for c in range(chunks):
        step_out_all[c * HEADS_AT_ONCE : (c + 1) * HEADS_AT_ONCE, :] = step_buf[c, :HEADS_AT_ONCE, :]
    for c in range(chunks):
        copy(c).wait()


def last_kernel(own, own_slope, x_taps, *rest):
    gets, rows_out, taps_out = rest[:-2], rest[-2], rest[-1]
    share = own_slope.shape[0]
    channels = x_taps.shape[1]
    parts = [own[...]] + [
        jnp.concatenate([get[0:share, :].astype(F32), joined_rows(get[share:, :])], 0)
        for get in gets
    ]
    total = tree_sum(parts)
    rows_out[...] = total[0:share] * own_slope[...]
    taps_out[:, :channels] = x_taps[...]
    taps_out[:, channels:] = total[share : share + taps_out.shape[0]]


def finish_kernel(bc_taps, own_rows, next_rows, sums, got, rows_out, x_taps_out, bc_taps_out, ext):
    share = own_rows.shape[0]
    ext[0:share, :] = own_rows[...]
    ext[share:, :] = next_rows[...]
    out = bc_taps[0:1, :] * ext[0:share, :]
    for k in range(1, bc_taps.shape[0]):
        out = out + bc_taps[k : k + 1, :] * ext[k : k + share, :]
    rows_out[...] = out
    total = sums[...] + got[...]
    channels = x_taps_out.shape[1]
    x_taps_out[...] = total[:, :channels]
    bc_taps_out[...] = total[:, channels:]


def local(xraw, zgate, bcraw, dt, a_rate, d_skip, conv_x, conv_bc, dout):
    length, channels = xraw.shape
    heads = a_rate.shape[0]
    n2 = bcraw.shape[1]
    n = n2 // 2
    taps = conv_x.shape[0]
    blocks = length // GROUP
    chunks = channels // WIDE
    count = lax.axis_size("seq")
    shares = lax.axis_size("head")
    share = length // shares
    place = jnp.stack([lax.axis_index("seq"), lax.axis_index("head")]).astype(jnp.int32)

    scalar = pl.BlockSpec(memory_space=pltpu.SMEM)
    local_ref = pl.BlockSpec(memory_space=pltpu.VMEM)
    far_ref = pl.BlockSpec(memory_space=pl.ANY)

    def arr(shape, dtype):
        return jax.ShapeDtypeStruct(shape, dtype)

    def far(value):
        return pltpu.with_memory_space_constraint(value, pltpu.HBM)

    def near(value):
        return pltpu.with_memory_space_constraint(value, pltpu.VMEM)

    params = pltpu.CompilerParams(vmem_limit_bytes=18 * 1024 * 1024)
    cover = pl.CostEstimate(
        flops=40_000_000_000, transcendentals=0, bytes_accessed=30_000_000
    )
    ext_x = pltpu.VMEM((HALVES, length + EDGE, LANES), F32)
    ext_bc = pltpu.VMEM((n2 // LANES, length + EDGE, LANES), F32)
    slabs = (chunks, length, WIDE)
    final = arr((length, channels), BF16)
    wide = pltpu.VMEM(slabs, BF16)
    stack = pltpu.VMEM((chunks, blocks, n, WIDE), BF16)
    xraw, zgate, dout = far(xraw), far(zgate), far(dout)
    square = (blocks, GROUP, GROUP)
    pairs = arr((chunks, 2 * HEADS_AT_ONCE, length), F32)

    def call(kernel, name, specs, out_shape, out_specs=None, scratch=(), covers=False):
        return pl.pallas_call(
            kernel,
            in_specs=specs,
            out_specs=out_specs or jax.tree.map(lambda _: local_ref, out_shape),
            out_shape=out_shape,
            scratch_shapes=list(scratch),
            compiler_params=params,
            cost_estimate=cover if covers else None,
            name=name,
        )

    last = length // RIM - 1
    rim_rows, steps, within = pl.pallas_call(
        prep_kernel,
        grid=(1,),
        in_specs=[scalar, pl.BlockSpec((RIM, channels), lambda c: (last, 0)),
                  pl.BlockSpec((RIM, n2), lambda c: (last, 0)),
                  pl.BlockSpec((heads, length), lambda c: (0, 0))],
        out_specs=[pl.BlockSpec((RIM, channels + n2), lambda c: (0, 0))]
        + [pl.BlockSpec(pairs.shape, lambda c: (0, 0, 0))] * 2,
        out_shape=[arr((RIM, channels + n2), BF16), pairs, pairs],
        compiler_params=params,
        name="prep",
    )(a_rate, xraw, far(bcraw), far(dt))
    before = from_behind(rim_rows, "seq", 1)
    gated = call(
        gate_kernel, "gate", [far_ref] * 3 + [local_ref] * 2,
        [pltpu.VMEM((length, channels), BF16)] + [wide] * 3
        + [pltpu.VMEM((chunks, length, 2 * HEADS_AT_ONCE), F32)],
        scratch=[pltpu.VMEM((blocks, GROUP, channels), BF16)] * 2
        + [pltpu.SemaphoreType.DMA((3, blocks))],
        covers=True,
    )(xraw, zgate, dout, steps, within)
    x, d, dy, gz, columns = map(near, gated)

    first = call(
        functools.partial(first_kernel, count), "first", [scalar] + [local_ref] * 8,
        [wide, arr((length, n2), BF16), arr(square, BF16), arr(square, BF16), stack, stack]
        + [arr((chunks, n + RIM, WIDE), BF16)] * (count - 1),
        scratch=[ext_x, ext_bc, pltpu.VMEM((blocks, n2, GROUP), BF16),
                 pltpu.VMEM((blocks, n, WIDE), F32)],
    )(place, before, x, bcraw, columns, within, conv_x, conv_bc, d)
    w, bc, lower, upper, states, grads = first[:6]
    w, states, grads = map(near, (w, states, grads))
    gets = [shifted(sent, "seq", k + 1) for k, sent in enumerate(first[6:])]

    inner = call(
        inner_kernel, "inner", [scalar] + [local_ref] * 13,
        [wide] * 5 + [pairs, arr((length, n2), F32), arr((length, n2), F32)],
        scratch=[ext_x, ext_bc, pltpu.VMEM(square, F32), pltpu.VMEM((GROUP, WIDE), BF16)],
        covers=True,
    )(d_skip, before, x, bcraw, conv_x, conv_bc, bc, lower, upper, dy, gz, columns, w, d)
    gate_base, gate_scale, slope_base, slope_scale, post = map(near, inner[:5])
    step_part, bc_part, bc_slope = inner[5:]

    half = shares // 2 * share + RIM
    shared = call(
        functools.partial(shared_kernel, count, shares, taps), "shared",
        [scalar] + [local_ref] * (11 + count),
        [stack, stack, arr((half, n2), F32), arr((share, n2), F32), arr((half, n2), BF16),
         arr((EDGE, channels), F32)],
        scratch=[pltpu.VMEM((length, n2), F32), ext_bc],
    )(place, before, bcraw, bc_slope, bc_part, bc, within, w, d, states, grads, slope_base,
      slope_scale, *gets)
    s_in, g_in, own, own_slope, sent, head_rows = shared
    s_in, g_in = near(s_in), near(g_in)
    x_next = from_behind(head_rows, "seq", -1)
    got = swapped(sent, "head", 1)

    gate_grad = call(
        gate_out_kernel, "gate_out", [local_ref] * 4, final, far_ref,
        scratch=[pltpu.VMEM(slabs, BF16), pltpu.SemaphoreType.DMA((chunks,))],
        covers=True,
    )(gate_base, gate_scale, bc, s_in)

    merged = call(
        merge_kernel, "merge", [scalar, local_ref, local_ref],
        [arr((share + RIM, n2), F32)] + [arr((share + RIM, n2), BF16)] * (shares // 2 - 1),
    )(place, own, got)
    own_parts = [swapped(part, "head", 2 * j + 2) for j, part in enumerate(merged[1:])]

    x_raw_grad, step_grad, x_taps_part = call(
        outer_kernel, "outer", [local_ref] * 4 + [far_ref] + [local_ref] * 7,
        [final, arr((heads, length), F32), arr((taps, channels), F32)],
        [far_ref, local_ref, local_ref],
        scratch=[ext_x, ext_x, pltpu.VMEM((GROUP, WIDE), BF16), pltpu.VMEM(slabs, BF16),
                 pltpu.VMEM(pairs.shape, F32), pltpu.SemaphoreType.DMA((chunks,))],
        covers=True,
    )(before, conv_x, bc, x_next, merged[0], x, within, slope_base, slope_scale, post, step_part,
      g_in)

    own_rows, tap_rows = call(
        last_kernel, "last", [local_ref] * (2 + shares // 2),
        [arr((share, n2), F32), arr((taps, channels + n2), F32)],
    )(merged[0], own_slope, x_taps_part, *own_parts)

    next_rows = from_behind(own_rows[:EDGE], ("seq", "head"), -1)
    sums, other = sum_over(tap_rows, "seq")
    bc_raw_grad, conv_x_grad, conv_bc_grad = call(
        finish_kernel, "finish", [local_ref] * 5,
        [arr((share, n2), F32), arr((taps, channels), F32), arr((taps, n2), F32)],
        scratch=[pltpu.VMEM((share + EDGE, n2), F32)],
    )(conv_bc, own_rows, next_rows, sums, other)
    return (x_raw_grad, gate_grad, step_grad, bc_raw_grad, conv_x_grad, conv_bc_grad)


def solution(mesh):
    placed = (
        P("seq", "head"),
        P("seq", "head"),
        P("seq", None),
        P("head", "seq"),
        P("head"),
        P("head"),
        P(None, "head"),
        P(),
        P("seq", "head"),
    )
    return jax.shard_map(
        local,
        mesh=mesh,
        in_specs=placed,
        out_specs=(
            P("seq", "head"),
            P("seq", "head"),
            P("head", "seq"),
            P(("seq", "head"), None),
            P(None, "head"),
            P(),
        ),
        check_vma=False,
    )
```

```python
import functools

import jax
import jax.numpy as jnp
from jax import lax
from jax.experimental import pallas as pl
from jax.experimental.pallas import tpu as pltpu
from jax.sharding import PartitionSpec as P

HEAD_DIM = 64
GROUP = 256
HEADS_AT_ONCE = 4
WIDE = HEAD_DIM * HEADS_AT_ONCE
LANES = 2 * HEAD_DIM
HALVES = HEADS_AT_ONCE // 2
SUB = 128
EDGE = 8
RIM = 16
F32 = jnp.float32
BF16 = jnp.bfloat16


def shifted(value, axis, steps):
    count = lax.axis_size(axis)
    return lax.ppermute(value, axis, [(i, (i + steps) % count) for i in range(count)])


def from_behind(value, axis, steps):
    count = lax.axis_size(axis)
    first, last = (max(0, -steps), min(count, count - steps))
    return lax.ppermute(value, axis, [(i, i + steps) for i in range(first, last)])


def swapped(value, axis, k):
    return lax.ppermute(value, axis, [(i, i ^ k) for i in range(lax.axis_size(axis))])


def tree_sum(parts):
    while len(parts) > 1:
        parts = [a + b for a, b in zip(parts[::2], parts[1::2])]
    return parts[0]


def sum_over(value, axis):
    k = 1
    while 2 * k < lax.axis_size(axis):
        value = value + swapped(value, axis, k)
        k *= 2
    return value, swapped(value, axis, k)


def dot(a, b):
    return jnp.dot(a, b, preferred_element_type=F32)


def dot_t(a, b):
    return lax.dot_general(a, b, (((1,), (1,)), ((), ())), preferred_element_type=F32)


def running_sum(g):
    place = lax.broadcasted_iota(jnp.int32, g.shape, 1) % GROUP
    step = 1
    while step < GROUP:
        g = g + jnp.where(place >= step, pltpu.roll(g, step, axis=1), 0.0)
        step *= 2
    return g


def token_gaps(within, k):
    w = within[:, rows_of(k)]
    total = w[:, GROUP - 1 : GROUP]
    return w - 0.5 * total, total


def token_columns(within, steps, k):
    gap, _ = token_gaps(within, k)
    upper = lax.broadcasted_iota(jnp.int32, gap.shape, 0) < HEADS_AT_ONCE
    e = jnp.exp(jnp.where(upper, gap, -gap))
    return jnp.where(upper, e * steps[:, rows_of(k)], e).T


def over_lanes(columns, first, h):
    rows = columns.shape[0]
    left = lax.broadcasted_iota(jnp.int32, (rows, LANES), 1) < HEAD_DIM
    a, b = (
        jnp.broadcast_to(columns[:, first + 2 * h + j : first + 2 * h + j + 1], (rows, LANES))
        for j in range(2)
    )
    return jnp.where(left, a, b)


def head_row(values):
    lane = lax.broadcasted_iota(jnp.int32, (1, WIDE), 1)
    row = jnp.broadcast_to(values[0], (1, WIDE))
    for j in range(1, HEADS_AT_ONCE):
        row = jnp.where(lane >= j * HEAD_DIM, jnp.broadcast_to(values[j], (1, WIDE)), row)
    return row


def total_row(total):
    return head_row([total[j : j + 1] for j in range(HEADS_AT_ONCE)])


def scalar_row(values, chunk):
    return head_row([values[chunk * HEADS_AT_ONCE + j] for j in range(HEADS_AT_ONCE)])


def load_extended(ext, rim, body):
    for h in range(body.shape[1] // LANES):
        lanes = slice(h * LANES, (h + 1) * LANES)
        ext[h, 0:EDGE, :] = rim[RIM - EDGE :, lanes].astype(F32)
        ext[h, EDGE : EDGE + body.shape[0], :] = body[:, lanes].astype(F32)


def behind(ext, h, start, k):
    return ext[h, EDGE + start - k : EDGE + start - k + SUB, :]


def conv_rows(ext, taps, h, start):
    lanes = slice(h * LANES, (h + 1) * LANES)
    out = taps[0:1, lanes] * behind(ext, h, start, 0)
    for k in range(1, taps.shape[0]):
        out = out + taps[k : k + 1, lanes] * behind(ext, h, start, k)
    return out


def silu_parts(half):
    t = jnp.tanh(half)
    a = 1.0 + t
    silu = half * a
    return silu, a + silu * (1.0 - t)


def silu_of(half):
    return half + half * jnp.tanh(half)


def pieces(k):
    for s in range(0, GROUP, SUB):
        for h in range(HALVES):
            here = k * GROUP + s
            yield slice(here, here + SUB), slice(h * LANES, (h + 1) * LANES), slice(s, s + SUB), h


def head_picks():
    shape = (WIDE, LANES)
    return (
        lax.broadcasted_iota(jnp.int32, shape, 0) // HEAD_DIM
        == lax.broadcasted_iota(jnp.int32, shape, 1)
    ).astype(BF16)


def chunk_lanes(c):
    return pl.ds(pl.multiple_of(c * WIDE, WIDE), WIDE)


def rows_of(k):
    if isinstance(k, int):
        return slice(k * GROUP, (k + 1) * GROUP)
    return pl.ds(pl.multiple_of(k * GROUP, GROUP), GROUP)


def prep_kernel(x, bcraw, rim, sems):
    length, channels = x.shape
    tail = pl.ds(length - RIM, RIM)
    one = pltpu.make_async_copy(x.at[tail, :], rim.at[:, :channels], sems.at[0])
    two = pltpu.make_async_copy(bcraw.at[tail, :], rim.at[:, channels:], sems.at[1])
    one.start()
    two.start()
    one.wait()
    two.wait()


def token_sums(rates, dt, steps_out, within_out):
    row = lax.broadcasted_iota(jnp.int32, steps_out.shape[1:], 0)
    for c in range(steps_out.shape[0]):
        steps = dt[c * HEADS_AT_ONCE : (c + 1) * HEADS_AT_ONCE, :]
        steps = jnp.concatenate([steps, steps], axis=0)
        rate = jnp.zeros(steps.shape, F32)
        for j in range(HEADS_AT_ONCE):
            rate = jnp.where(row % HEADS_AT_ONCE == j, rates[c * HEADS_AT_ONCE + j], rate)
        steps_out[c] = steps
        within_out[c] = running_sum(rate * steps)


def gate_kernel(
    rates, x, z, up, dt, x_out, d_out, dy_out, gz_out, columns_out, within, z_buf, up_buf, steps,
    sems,
):
    chunks = d_out.shape[0]
    blocks = z_buf.shape[0]

    def copy(j, k):
        source, target = ((z, z_buf.at[k]), (up, up_buf.at[k]), (x, x_out.at[rows_of(k), :]))[j]
        return pltpu.make_async_copy(source.at[rows_of(k), :], target, sems.at[j, k])

    for k in range(blocks):
        copy(0, k).start()
        copy(1, k).start()
    for k in range(blocks):
        copy(2, k).start()
    token_sums(rates, dt, steps, within)

    @pl.loop(0, blocks)
    def _(k):
        copy(0, k).wait()
        copy(1, k).wait()
        for c in range(chunks):
            columns = token_columns(within.at[c], steps.at[c], k)
            columns_out[c, rows_of(k), :] = columns
            for part_rows, lanes, part, h in pieces(0):
                here = slice(c * WIDE + lanes.start, c * WIDE + lanes.stop)
                rows = pl.ds(pl.multiple_of(k * GROUP + part.start, SUB), SUB)
                silu, slope = silu_parts(0.5 * z_buf[k, part, here].astype(F32))
                upstream = up_buf[k, part, here].astype(F32)
                dy = (upstream * silu).astype(BF16)
                dy_out[c, rows, lanes] = dy
                gz_out[c, rows, lanes] = (upstream * slope).astype(BF16)
                v = over_lanes(columns[part], HEADS_AT_ONCE, h)
                d_out[c, rows, lanes] = (v * dy.astype(F32)).astype(BF16)

    for k in range(blocks):
        copy(2, k).wait()


def gate_out_kernel(gate_base, gate_scale, bc, s_in, gate_out, buf, sems):
    chunks = buf.shape[0]
    n = s_in.shape[2]

    def copy(c):
        return pltpu.make_async_copy(buf.at[c], gate_out.at[:, chunk_lanes(c)], sems.at[c])

    @pl.loop(0, chunks)
    def _(c):
        for k in range(bc.shape[0] // GROUP):
            y1 = dot(bc[rows_of(k), n:], s_in[c, k])
            for rows, lanes, part, h in pieces(k):
                buf[c, rows, lanes] = (
                    gate_base[c, rows, lanes].astype(F32)
                    + gate_scale[c, rows, lanes].astype(F32) * y1[part, lanes]
                ).astype(BF16)
        copy(c).start()

    for c in range(chunks):
        copy(c).wait()


def first_kernel(
    count, place, rims, x_all, bcraw, columns_all, within_all, taps, bc_taps, d_all,
    w_all, bc_out, lower, upper, states_all, grads_all, *rest,
):
    sends_all = rest[: count - 1]
    ext, bc_ext, bct, ctd = rest[count - 1 :]
    length = bcraw.shape[0]
    blocks = length // GROUP
    n = bcraw.shape[1] // 2
    channels = taps.shape[1]

    load_extended(bc_ext, rims.at[:, channels:], bcraw)
    bc_half = 0.5 * bc_taps[...]
    r = lax.broadcasted_iota(jnp.int32, (GROUP, GROUP), 0)
    c = lax.broadcasted_iota(jnp.int32, (GROUP, GROUP), 1)
    for k in range(blocks):
        for rows, lanes, part, h in pieces(k):
            post = silu_of(conv_rows(bc_ext, bc_half, h, rows.start)).astype(BF16)
            bc_out[rows, lanes] = post
            bct[k, lanes, part] = post.astype(F32).T.astype(BF16)
        b, cc = bc_out[rows_of(k), :n], bc_out[rows_of(k), n:]
        lower[k] = jnp.where(r >= c, dot(cc, bct[k, :n, :]), 0.0).astype(BF16)
        upper[k] = jnp.where(r <= c, dot(b, bct[k, n:, :]), 0.0).astype(BF16)

    @pl.loop(0, w_all.shape[0])
    def _(c):
        columns, within, d, w_out, states, grads = (
            ref.at[c] for ref in (columns_all, within_all, d_all, w_all, states_all, grads_all)
        )
        x = x_all.at[:, chunk_lanes(c)]
        sends = [ref.at[c] for ref in sends_all]
        load_extended(ext, rims.at[:, chunk_lanes(c)], x)
        half_taps = 0.5 * taps[:, chunk_lanes(c)]
        state = jnp.zeros((n, WIDE), F32)
        totals = []
        for k in range(blocks):
            _, total = token_gaps(within, k)
            for rows, lanes, part, h in pieces(k):
                post = silu_of(conv_rows(ext, half_taps, h, rows.start)).astype(BF16).astype(F32)
                w_out[rows, lanes] = (over_lanes(columns[rows, :], 0, h) * post).astype(BF16)
            total = total_row(total)
            totals.append(total)
            states[k] = state.astype(BF16)
            half = jnp.exp(-0.5 * total)
            state = jnp.exp(-total) * state + half * dot(bct[k, :n, :], w_out[rows_of(k), :])
            ctd[k] = half * dot(bct[k, n:, :], d[rows_of(k), :])
        grad = jnp.zeros((n, WIDE), F32)
        for k in reversed(range(blocks)):
            grads[k] = grad.astype(BF16)
            grad = jnp.exp(-totals[k]) * grad + ctd[k]
        whole = sum(totals[1:], totals[0])
        high = whole.astype(BF16).astype(F32)
        mid = (whole - high).astype(BF16).astype(F32)
        low = whole - high - mid
        r = lax.broadcasted_iota(jnp.int32, (RIM, WIDE), 0)
        extra = jnp.where(r == 0, high, jnp.where(r == 1, mid, jnp.where(r == 2, low, 0.0))).astype(BF16)
        for k in range(1, count):
            onward = place[0] + k < count
            sends[k - 1][0:n, :] = jnp.where(onward, state, grad).astype(BF16)
            sends[k - 1][n:, :] = extra


def inner_kernel(
    skips, rims, x_all, bcraw, taps, bc_taps, bc, lower, upper,
    dy_all, gz_all, columns_all, w_all, d_all,
    gate_base_all, gate_scale_all, slope_base_all, slope_scale_all, post_all, step_all,
    bc_part, bc_slope, ext, bc_ext, mix, quick,
):
    channels = taps.shape[1]
    blocks = bc.shape[0] // GROUP
    n = bc.shape[1] // 2
    mix[...] = jnp.zeros_like(mix)
    picks = head_picks()

    @pl.loop(0, w_all.shape[0])
    def _(c):
        dy, gz, columns, w, d = (
            ref.at[c] for ref in (dy_all, gz_all, columns_all, w_all, d_all)
        )
        x = x_all.at[:, chunk_lanes(c)]
        gate_base, gate_scale, slope_base, slope_scale, post_out, step_out = (
            ref.at[c]
            for ref in (gate_base_all, gate_scale_all, slope_base_all, slope_scale_all, post_all,
                        step_all)
        )
        load_extended(ext, rims.at[:, chunk_lanes(c)], x)
        half_taps = 0.5 * taps[:, chunk_lanes(c)]
        half_skip = 0.5 * scalar_row(skips, c)
        for k in range(blocks):
            y0 = dot(lower[k], w[rows_of(k), :])
            p0 = dot(upper[k], d[rows_of(k), :])
            mix[k] += dot_t(d[rows_of(k), :], w[rows_of(k), :])
            for rows, lanes, part, h in pieces(k):
                silu, slope = silu_parts(conv_rows(ext, half_taps, h, rows.start))
                post_b = silu.astype(BF16)
                post = post_b.astype(F32)
                post_out[rows, lanes] = post_b
                skip = half_skip[:, lanes]
                scales = 0.5 * columns[rows, :]
                v = over_lanes(scales, HEADS_AT_ONCE, h)
                gate = gz[rows, lanes].astype(F32)
                gate_base[rows, lanes] = (gate * (v * y0[part, lanes] + skip * post)).astype(BF16)
                gate_scale[rows, lanes] = (gate * v).astype(BF16)
                ud = over_lanes(scales, 0, h)
                p = p0[part, lanes]
                slope_base[rows, lanes] = (
                    slope * (ud * p + skip * dy[rows, lanes].astype(F32))
                ).astype(BF16)
                slope_scale[rows, lanes] = (slope * ud).astype(BF16)
                quick[part, lanes] = (post * p).astype(BF16)
            step_out[:, rows_of(k)] = dot(quick[...], picks).T[: 2 * HEADS_AT_ONCE]

    load_extended(bc_ext, rims.at[:, channels:], bcraw)
    bc_half = 0.5 * bc_taps[...]
    r = lax.broadcasted_iota(jnp.int32, (GROUP, GROUP), 0)
    c = lax.broadcasted_iota(jnp.int32, (GROUP, GROUP), 1)
    for k in range(blocks):
        m = jnp.where(r >= c, mix[k], 0.0)
        bc_part[rows_of(k), n:] = dot(m.astype(BF16), bc[rows_of(k), :n])
        bc_part[rows_of(k), :n] = dot(m.T.astype(BF16), bc[rows_of(k), n:])
        for rows, lanes, part, h in pieces(k):
            bc_slope[rows, lanes] = 0.5 * silu_parts(conv_rows(bc_ext, bc_half, h, rows.start))[1]


def shared_kernel(
    count, shares, tap_count, place, rims, bcraw, bc_slope, bc_part, bc,
    within_all, w_all, d_all, states_all, grads_all, slope_base_all, slope_scale_all, *rest,
):
    gets_all = rest[: count - 1]
    s_all, g_all, own, own_slope, sent, heads_all, acc, bc_ext = rest[count - 1 :]
    length = bc.shape[0]
    blocks = length // GROUP
    n = bcraw.shape[1] // 2
    channels = heads_all.shape[1]
    acc[...] = bc_part[...]

    @pl.loop(0, w_all.shape[0])
    def _(c):
        within, w, d, states, grads, slope_base, slope_scale, s_out, g_out = (
            ref.at[c]
            for ref in (within_all, w_all, d_all, states_all, grads_all, slope_base_all,
                        slope_scale_all, s_all, g_all)
        )
        gets = [ref.at[c] for ref in gets_all]
        state_in = jnp.zeros((n, WIDE), F32)
        grad_in = jnp.zeros((n, WIDE), F32)
        spans = [None] + [
            sum(get[n + j : n + j + 1, :].astype(F32) for j in range(3)) for get in gets
        ]
        gone = jnp.zeros((1, WIDE), F32)
        for k in range(1, count):
            weight = jnp.where(place[0] >= k, jnp.exp(-gone), 0.0)
            state_in = state_in + weight * gets[k - 1][0:n, :].astype(F32)
            gone = gone + spans[k]
        gone = jnp.zeros((1, WIDE), F32)
        for ahead in range(1, count):
            k = count - ahead
            weight = jnp.where(place[0] < k, jnp.exp(-gone), 0.0)
            grad_in = grad_in + weight * gets[k - 1][0:n, :].astype(F32)
            gone = gone + spans[k]
        totals = [
            total_row(within[:, (k + 1) * GROUP - 1 : (k + 1) * GROUP]) for k in range(blocks)
        ]
        gone = jnp.zeros((1, WIDE), F32)
        for k in range(blocks):
            half = jnp.exp(-0.5 * totals[k])
            later = sum(totals[k + 1 :], jnp.zeros((1, WIDE), F32))
            sk = (half * (states[k].astype(F32) + jnp.exp(-gone) * state_in)).astype(BF16)
            gk = (half * (grads[k].astype(F32) + jnp.exp(-later) * grad_in)).astype(BF16)
            gone = gone + totals[k]
            s_out[k] = sk
            g_out[k] = gk
            if k == 0:
                p = dot(bc[0:RIM, :n], gk)[0:EDGE]
                heads_all[:, chunk_lanes(c)] = (
                    slope_base[0:EDGE, :].astype(F32) + slope_scale[0:EDGE, :].astype(F32) * p
                )
            acc[rows_of(k), n:] += dot_t(d[rows_of(k), :], sk)
            acc[rows_of(k), :n] += dot_t(w[rows_of(k), :], gk)

    load_extended(bc_ext, rims.at[:, channels:], bcraw)
    share = length // shares
    taps = tap_count
    sums = {}
    for k in range(blocks):
        for rows, lanes, part, h in pieces(k):
            full = bc_slope[rows, lanes] * acc[rows, lanes]
            for j in range(taps):
                fresh = jnp.sum(
                    (full * behind(bc_ext, h, rows.start, j)).reshape(SUB // 8, 8, LANES), axis=0
                )
                sums[h, j] = sums[h, j] + fresh if (h, j) in sums else fresh
    halves = []
    for h in range(HALVES):
        halves.append([jnp.sum(sums[h, j], axis=0, keepdims=True) for j in range(taps)])
    rows = shares // 2 * share
    own[rows:, :] = jnp.zeros((RIM, 2 * n), F32)
    for j in range(taps):
        for h in range(HALVES):
            own[rows + j : rows + j + 1, h * LANES : (h + 1) * LANES] = halves[h][j]
    sent[rows:, :] = split_rows(own[rows:, :])
    own[rows:, :] = joined_rows(split_rows(own[rows:, :]))
    core = lax.rem(place[1], 2)
    own_slope[...] = bc_slope[pl.ds(pl.multiple_of(place[1] * share, share), share), :]
    for j in range(shares // 2):
        here = slice(j * share, (j + 1) * share)
        start = pl.multiple_of((2 * j + core) * share, share)
        own[here, :] = acc[pl.ds(start, share), :]
        start = pl.multiple_of((2 * j + 1 - core) * share, share)
        sent[here, :] = acc[pl.ds(start, share), :].astype(BF16)


def split_rows(rows):
    high = rows.astype(BF16).astype(F32)
    return (high + pltpu.roll(rows - high, RIM // 2, axis=0)).astype(BF16)


def joined_rows(rows):
    rows = rows.astype(F32)
    return rows + pltpu.roll(rows, RIM // 2, axis=0)


def merge_kernel(place, own, get, mine, *sends):
    share = mine.shape[0] - RIM
    rows = own.shape[0] - RIM
    far_place = lax.div(place[1], 2)
    place_rows = lax.broadcasted_iota(jnp.int32, (RIM, own.shape[1]), 0)
    taps = own[rows:, :] + joined_rows(get[rows:, :])
    packed = split_rows(jnp.where(place_rows < RIM // 2, taps, 0.0))
    start = pl.multiple_of(far_place * share, share)
    mine[0:share, :] = own[pl.ds(start, share), :] + get[pl.ds(start, share), :].astype(F32)
    mine[share:, :] = joined_rows(packed)
    for j in range(1, len(sends) + 1):
        start = pl.multiple_of(lax.bitwise_xor(far_place, jnp.int32(j)) * share, share)
        total = own[pl.ds(start, share), :] + get[pl.ds(start, share), :].astype(F32)
        sends[j - 1][0:share, :] = total.astype(BF16)
        sends[j - 1][share:, :] = packed


def outer_kernel(
    rims, taps_all, bc, x_next, after, x_all, within_all, slope_base_all, slope_scale_all, post_all,
    steps_all, g_all, x_out_all, step_out_all, tap_part, ext, slope_ext, quick, buf, step_buf, sems,
):
    length = bc.shape[0]
    blocks = length // GROUP
    n = g_all.shape[2]
    count = taps_all.shape[0]
    chunks = buf.shape[0]
    picks = head_picks()

    def copy(c):
        return pltpu.make_async_copy(buf.at[c], x_out_all.at[:, chunk_lanes(c)], sems.at[c])

    @pl.loop(0, chunks)
    def _(c):
        x = x_all.at[:, chunk_lanes(c)]
        within, slope_base, slope_scale, post, step_part, g_in, x_out, step_out = (
            ref.at[c]
            for ref in (within_all, slope_base_all, slope_scale_all, post_all, steps_all,
                        g_all, buf, step_buf)
        )
        load_extended(ext, rims.at[:, chunk_lanes(c)], x)
        taps = taps_all[:, chunk_lanes(c)]
        following = x_next[:, chunk_lanes(c)]
        sums = {}
        for h in range(HALVES):
            slope_ext[h, length : length + EDGE, :] = following[:, h * LANES : (h + 1) * LANES]
        for k in range(blocks):
            p1 = dot(bc[rows_of(k), :n], g_in[k])
            for rows, lanes, part, h in pieces(k):
                p = p1[part, lanes]
                slope = slope_base[rows, lanes].astype(F32) + slope_scale[rows, lanes].astype(F32) * p
                slope_ext[h, rows, :] = slope
                for j in range(count):
                    fresh = jnp.sum(
                        (slope * behind(ext, h, rows.start, j)).reshape(SUB // 8, 8, LANES), axis=0
                    )
                    sums[h, j] = sums[h, j] + fresh if (h, j) in sums else fresh
                quick[part, lanes] = (post[rows, lanes].astype(F32) * p).astype(BF16)
            st = dot(quick[...], picks).T[: 2 * HEADS_AT_ONCE]
            step_out[:, rows_of(k)] = jnp.exp(token_gaps(within, k)[0]) * (st + step_part[:, rows_of(k)])
        tap_part[:, chunk_lanes(c)] = jnp.concatenate(
            [
                jnp.concatenate(
                    [jnp.sum(sums[h, j], axis=0, keepdims=True) for h in range(HALVES)], axis=1
                )
                for j in range(count)
            ],
            axis=0,
        )
        for h in range(HALVES):
            lanes = slice(h * LANES, (h + 1) * LANES)
            for s in range(0, length, SUB):
                out = taps[0:1, lanes] * slope_ext[h, s : s + SUB, :]
                for j in range(1, count):
                    out = out + taps[j : j + 1, lanes] * slope_ext[h, s + j : s + j + SUB, :]
                x_out[s : s + SUB, lanes] = out.astype(BF16)
        copy(c).start()

    for c in range(chunks):
        step_out_all[c * HEADS_AT_ONCE : (c + 1) * HEADS_AT_ONCE, :] = step_buf[c, :HEADS_AT_ONCE, :]
    for c in range(chunks):
        copy(c).wait()


def last_kernel(own, own_slope, x_taps, *rest):
    gets, rows_out, taps_out = rest[:-2], rest[-2], rest[-1]
    share = own_slope.shape[0]
    channels = x_taps.shape[1]
    parts = [own[...]] + [
        jnp.concatenate([get[0:share, :].astype(F32), joined_rows(get[share:, :])], 0)
        for get in gets
    ]
    total = tree_sum(parts)
    rows_out[...] = total[0:share] * own_slope[...]
    taps_out[:, :channels] = x_taps[...]
    taps_out[:, channels:] = total[share : share + taps_out.shape[0]]


def finish_kernel(bc_taps, own_rows, next_rows, sums, got, rows_out, x_taps_out, bc_taps_out, ext):
    share = own_rows.shape[0]
    ext[0:share, :] = own_rows[...]
    ext[share:, :] = next_rows[...]
    out = bc_taps[0:1, :] * ext[0:share, :]
    for k in range(1, bc_taps.shape[0]):
        out = out + bc_taps[k : k + 1, :] * ext[k : k + share, :]
    rows_out[...] = out
    total = sums[...] + got[...]
    channels = x_taps_out.shape[1]
    x_taps_out[...] = total[:, :channels]
    bc_taps_out[...] = total[:, channels:]


def local(xraw, zgate, bcraw, dt, a_rate, d_skip, conv_x, conv_bc, dout):
    length, channels = xraw.shape
    heads = a_rate.shape[0]
    n2 = bcraw.shape[1]
    n = n2 // 2
    taps = conv_x.shape[0]
    blocks = length // GROUP
    chunks = channels // WIDE
    count = lax.axis_size("seq")
    shares = lax.axis_size("head")
    share = length // shares
    place = jnp.stack([lax.axis_index("seq"), lax.axis_index("head")]).astype(jnp.int32)

    scalar = pl.BlockSpec(memory_space=pltpu.SMEM)
    local_ref = pl.BlockSpec(memory_space=pltpu.VMEM)
    far_ref = pl.BlockSpec(memory_space=pl.ANY)

    def arr(shape, dtype):
        return jax.ShapeDtypeStruct(shape, dtype)

    def far(value):
        return pltpu.with_memory_space_constraint(value, pltpu.HBM)

    def near(value):
        return pltpu.with_memory_space_constraint(value, pltpu.VMEM)

    params = pltpu.CompilerParams(vmem_limit_bytes=18 * 1024 * 1024)
    cover = pl.CostEstimate(
        flops=40_000_000_000, transcendentals=0, bytes_accessed=30_000_000
    )
    ext_x = pltpu.VMEM((HALVES, length + EDGE, LANES), F32)
    ext_bc = pltpu.VMEM((n2 // LANES, length + EDGE, LANES), F32)
    slabs = (chunks, length, WIDE)
    final = arr((length, channels), BF16)
    wide = pltpu.VMEM(slabs, BF16)
    stack = pltpu.VMEM((chunks, blocks, n, WIDE), BF16)
    xraw, zgate, dout = far(xraw), far(zgate), far(dout)
    square = (blocks, GROUP, GROUP)
    pairs = arr((chunks, 2 * HEADS_AT_ONCE, length), F32)

    def call(kernel, name, specs, out_shape, out_specs=None, scratch=(), covers=False):
        return pl.pallas_call(
            kernel,
            in_specs=specs,
            out_specs=out_specs or jax.tree.map(lambda _: local_ref, out_shape),
            out_shape=out_shape,
            scratch_shapes=list(scratch),
            compiler_params=params,
            cost_estimate=cover if covers else None,
            name=name,
        )

    rim_rows = call(
        prep_kernel, "prep", [far_ref, far_ref], arr((RIM, channels + n2), BF16), local_ref,
        scratch=[pltpu.SemaphoreType.DMA((2,))],
    )(xraw, far(bcraw))
    before = from_behind(rim_rows, "seq", 1)
    gated = call(
        gate_kernel, "gate", [scalar] + [far_ref] * 3 + [local_ref],
        [pltpu.VMEM((length, channels), BF16)] + [wide] * 3
        + [pltpu.VMEM((chunks, length, 2 * HEADS_AT_ONCE), F32), pairs],
        scratch=[pltpu.VMEM((blocks, GROUP, channels), BF16)] * 2
        + [pltpu.VMEM(pairs.shape, F32), pltpu.SemaphoreType.DMA((3, blocks))],
        covers=True,
    )(a_rate, xraw, zgate, dout, dt)
    x, d, dy, gz, columns = map(near, gated[:5])
    within = gated[5]

    first = call(
        functools.partial(first_kernel, count), "first", [scalar] + [local_ref] * 8,
        [wide, arr((length, n2), BF16), arr(square, BF16), arr(square, BF16), stack, stack]
        + [arr((chunks, n + RIM, WIDE), BF16)] * (count - 1),
        scratch=[ext_x, ext_bc, pltpu.VMEM((blocks, n2, GROUP), BF16),
                 pltpu.VMEM((blocks, n, WIDE), F32)],
    )(place, before, x, bcraw, columns, within, conv_x, conv_bc, d)
    w, bc, lower, upper, states, grads = first[:6]
    w, states, grads = map(near, (w, states, grads))
    gets = [shifted(sent, "seq", k + 1) for k, sent in enumerate(first[6:])]

    inner = call(
        inner_kernel, "inner", [scalar] + [local_ref] * 13,
        [wide] * 5 + [pairs, arr((length, n2), F32), arr((length, n2), F32)],
        scratch=[ext_x, ext_bc, pltpu.VMEM(square, F32), pltpu.VMEM((GROUP, WIDE), BF16)],
        covers=True,
    )(d_skip, before, x, bcraw, conv_x, conv_bc, bc, lower, upper, dy, gz, columns, w, d)
    gate_base, gate_scale, slope_base, slope_scale, post = map(near, inner[:5])
    step_part, bc_part, bc_slope = inner[5:]

    half = shares // 2 * share + RIM
    shared = call(
        functools.partial(shared_kernel, count, shares, taps), "shared",
        [scalar] + [local_ref] * (11 + count),
        [stack, stack, arr((half, n2), F32), arr((share, n2), F32), arr((half, n2), BF16),
         arr((EDGE, channels), F32)],
        scratch=[pltpu.VMEM((length, n2), F32), ext_bc],
    )(place, before, bcraw, bc_slope, bc_part, bc, within, w, d, states, grads, slope_base,
      slope_scale, *gets)
    s_in, g_in, own, own_slope, sent, head_rows = shared
    s_in, g_in = near(s_in), near(g_in)
    x_next = from_behind(head_rows, "seq", -1)
    got = swapped(sent, "head", 1)

    gate_grad = call(
        gate_out_kernel, "gate_out", [local_ref] * 4, final, far_ref,
        scratch=[pltpu.VMEM(slabs, BF16), pltpu.SemaphoreType.DMA((chunks,))],
        covers=True,
    )(gate_base, gate_scale, bc, s_in)

    merged = call(
        merge_kernel, "merge", [scalar, local_ref, local_ref],
        [arr((share + RIM, n2), F32)] + [arr((share + RIM, n2), BF16)] * (shares // 2 - 1),
    )(place, own, got)
    own_parts = [swapped(part, "head", 2 * j + 2) for j, part in enumerate(merged[1:])]

    x_raw_grad, step_grad, x_taps_part = call(
        outer_kernel, "outer", [local_ref] * 4 + [far_ref] + [local_ref] * 7,
        [final, arr((heads, length), F32), arr((taps, channels), F32)],
        [far_ref, local_ref, local_ref],
        scratch=[ext_x, ext_x, pltpu.VMEM((GROUP, WIDE), BF16), pltpu.VMEM(slabs, BF16),
                 pltpu.VMEM(pairs.shape, F32), pltpu.SemaphoreType.DMA((chunks,))],
        covers=True,
    )(before, conv_x, bc, x_next, merged[0], x, within, slope_base, slope_scale, post, step_part,
      g_in)

    own_rows, tap_rows = call(
        last_kernel, "last", [local_ref] * (2 + shares // 2),
        [arr((share, n2), F32), arr((taps, channels + n2), F32)],
    )(merged[0], own_slope, x_taps_part, *own_parts)

    next_rows = from_behind(own_rows[:EDGE], ("seq", "head"), -1)
    sums, other = sum_over(tap_rows, "seq")
    bc_raw_grad, conv_x_grad, conv_bc_grad = call(
        finish_kernel, "finish", [local_ref] * 5,
        [arr((share, n2), F32), arr((taps, channels), F32), arr((taps, n2), F32)],
        scratch=[pltpu.VMEM((share + EDGE, n2), F32)],
    )(conv_bc, own_rows, next_rows, sums, other)
    return (x_raw_grad, gate_grad, step_grad, bc_raw_grad, conv_x_grad, conv_bc_grad)


def solution(mesh):
    placed = (
        P("seq", "head"),
        P("seq", "head"),
        P("seq", None),
        P("head", "seq"),
        P("head"),
        P("head"),
        P(None, "head"),
        P(),
        P("seq", "head"),
    )
    return jax.shard_map(
        local,
        mesh=mesh,
        in_specs=placed,
        out_specs=(
            P("seq", "head"),
            P("seq", "head"),
            P("head", "seq"),
            P(("seq", "head"), None),
            P(None, "head"),
            P(),
        ),
        check_vma=False,
    )
```
